32 devices in a mesh: dp: 1 (over z), tp: 4 (over y), sp: 8 (over x, core).
Axes of the slice: x: 4, y: 4, z: 1, core: 2. Of those that a mesh axis runs over, the one named last changes fastest.
The devices are a block of a 4x4x8 slice.
Arguments:
- hidden: bfloat16 [256, 7168], P('dp')
- lat_cache: bfloat16 [256, 2048, 512], P('dp', 'sp')
- rope_cache: bfloat16 [256, 2048, 64], P('dp', 'sp')
- positions: int32 [256], P('dp')
- w_dq: bfloat16 [7168, 1536], replicated
- gain_q: bfloat16 [1536], replicated
- w_dkv: bfloat16 [7168, 576], replicated
- gain_kv: bfloat16 [512], replicated
- w_uq: bfloat16 [1536, 64, 192], P(None, 'tp')
- w_uk: bfloat16 [512, 64, 128], P(None, 'tp')
- w_uv: bfloat16 [512, 64, 128], P(None, 'tp')
- w_out: bfloat16 [8192, 7168], P('tp')
Outputs:
- output 1: bfloat16 [256, 7168], P('dp')
- output 2: bfloat16 [256, 2048, 512], P('dp', 'sp')
- output 3: bfloat16 [256, 2048, 64], P('dp', 'sp')
All inputs are finite; a program needn't handle non-finite values.
Results may differ from the reference program's by a relative error of at most 0.0115735.
Values sent between devices are 32-bit elements.
A program may use at most 768 MiB of HBM per device.

```python
import math
import jax
import jax.numpy as jnp
from jax import lax

BATCH = 256
SEQ = 2048
DMODEL = 7168
HEADS = 64
QRANK = 1536
KVRANK = 512
NOPE = 128
ROPE = 64
VHEAD = 128

EPSILON = 1e-6
ROPE_BASE = 50000.0
SCORE_SCALE = (1.0 + 0.1 * math.log(32.0)) ** 2 / math.sqrt(NOPE + ROPE)
LAT_SPREAD = 1.2
ROPE_SPREAD = 1.7


def setup_inputs(seed: int = 0, part: int = 0) -> dict:
    base_key = jax.random.key(seed)
    shared_keys = jax.random.split(base_key, 8)
    part_keys = jax.random.split(jax.random.fold_in(base_key, part), 5)
    hidden = jax.random.normal(part_keys[0], (BATCH, DMODEL), jnp.float32)
    lat_cache = LAT_SPREAD * jax.random.normal(part_keys[1], (BATCH, SEQ, KVRANK), jnp.float32)
    rope_cache = ROPE_SPREAD * jax.random.normal(part_keys[2], (BATCH, SEQ, ROPE), jnp.float32)
    long_pos = jax.random.randint(part_keys[3], (BATCH,), 0, SEQ, jnp.int32)
    short_pos = jax.random.randint(part_keys[4], (BATCH,), 0, 4, jnp.int32)
    positions = jnp.where(jnp.arange(BATCH) % 4 == 1, short_pos, long_pos)
    positions = positions.at[0].set(SEQ - 1).at[1].set(0)
    w_dq = jax.random.normal(shared_keys[0], (DMODEL, QRANK), jnp.float32) * DMODEL ** -0.5
    gain_q = 1.0 + 0.5 * jax.random.normal(shared_keys[1], (QRANK,), jnp.float32)
    w_dkv = jax.random.normal(shared_keys[2], (DMODEL, KVRANK + ROPE), jnp.float32) * DMODEL ** -0.5
    gain_kv = 1.0 + 0.5 * jax.random.normal(shared_keys[3], (KVRANK,), jnp.float32)
    w_uq = jax.random.normal(shared_keys[4], (QRANK, HEADS, NOPE + ROPE), jnp.float32) * QRANK ** -0.5
    w_uk = jax.random.normal(shared_keys[5], (KVRANK, HEADS, NOPE), jnp.float32) * KVRANK ** -0.5
    w_uv = jax.random.normal(shared_keys[6], (KVRANK, HEADS, VHEAD), jnp.float32) * KVRANK ** -0.5
    w_out = jax.random.normal(shared_keys[7], (HEADS * VHEAD, DMODEL), jnp.float32) * (HEADS * VHEAD) ** -0.5
    return {
        'hidden': hidden.astype(jnp.bfloat16),
        'lat_cache': lat_cache.astype(jnp.bfloat16),
        'rope_cache': rope_cache.astype(jnp.bfloat16),
        'positions': positions,
        'w_dq': w_dq.astype(jnp.bfloat16),
        'gain_q': gain_q.astype(jnp.bfloat16),
        'w_dkv': w_dkv.astype(jnp.bfloat16),
        'gain_kv': gain_kv.astype(jnp.bfloat16),
        'w_uq': w_uq.astype(jnp.bfloat16),
        'w_uk': w_uk.astype(jnp.bfloat16),
        'w_uv': w_uv.astype(jnp.bfloat16),
        'w_out': w_out.astype(jnp.bfloat16),
    }


def rms_norm(values, gain):
    vals32 = values.astype(jnp.float32)
    inv_rms = lax.rsqrt(jnp.mean(vals32 * vals32, axis=-1, keepdims=True) + EPSILON)
    return vals32 * inv_rms * gain.astype(jnp.float32)


def rope_angles(positions):
    half_dim = ROPE // 2
    inv_freq = ROPE_BASE ** (-jnp.arange(half_dim).astype(jnp.float32) / half_dim)
    return positions.astype(jnp.float32)[:, None] * inv_freq[None, :]


def rotate_pairs(values, cos_t, sin_t):
    half_dim = values.shape[-1] // 2
    first_half = values[..., :half_dim]
    second_half = values[..., half_dim:]
    return jnp.concatenate([first_half * cos_t - second_half * sin_t, second_half * cos_t + first_half * sin_t], axis=-1)


def attend_one(operands):
    q_abs, q_rope, lat_all, rope_all, position = operands
    lat32 = lat_all.astype(jnp.float32)
    scores = (jnp.einsum('hk,sk->hs', q_abs.astype(jnp.float32), lat32) + jnp.einsum('hr,sr->hs', q_rope.astype(jnp.float32), rope_all.astype(jnp.float32))) * SCORE_SCALE
    key_valid = jnp.arange(SEQ)[None, :] <= position
    scores = jnp.where(key_valid, scores, -jnp.inf)
    probs = jax.nn.softmax(scores, axis=-1)
    return jnp.einsum('hs,sk->hk', probs, lat32).astype(jnp.bfloat16)


def reference(hidden, lat_cache, rope_cache, positions, w_dq, gain_q, w_dkv, gain_kv, w_uq, w_uk, w_uv, w_out):
    angles = rope_angles(positions)
    cos_t = jnp.cos(angles)
    sin_t = jnp.sin(angles)
    h_q = jnp.dot(hidden, w_dq, preferred_element_type=jnp.float32).astype(jnp.bfloat16)
    c_q = rms_norm(h_q, gain_q).astype(jnp.bfloat16)
    q_full = jnp.einsum('br,rhd->bhd', c_q.astype(jnp.float32), w_uq.astype(jnp.float32)).astype(jnp.bfloat16)
    q_nope = q_full[:, :, :NOPE]
    q_rope = rotate_pairs(q_full[:, :, NOPE:].astype(jnp.float32), cos_t[:, None, :], sin_t[:, None, :]).astype(jnp.bfloat16)
    kv_down = jnp.dot(hidden, w_dkv, preferred_element_type=jnp.float32).astype(jnp.bfloat16)
    lat_new = rms_norm(kv_down[:, :KVRANK], gain_kv).astype(jnp.bfloat16)
    rope_new = rotate_pairs(kv_down[:, KVRANK:].astype(jnp.float32), cos_t, sin_t).astype(jnp.bfloat16)
    slot_hit = (jnp.arange(SEQ)[None, :] == positions[:, None])[:, :, None]
    lat_all = jnp.where(slot_hit, lat_new[:, None, :], lat_cache)
    rope_all = jnp.where(slot_hit, rope_new[:, None, :], rope_cache)
    q_abs = jnp.einsum('bhn,khn->bhk', q_nope.astype(jnp.float32), w_uk.astype(jnp.float32)).astype(jnp.bfloat16)
    o_lat = lax.map(attend_one, (q_abs, q_rope, lat_all, rope_all, positions))
    o_heads = jnp.einsum('bhk,khv->bhv', o_lat.astype(jnp.float32), w_uv.astype(jnp.float32)).astype(jnp.bfloat16)
    attn_out = jnp.dot(o_heads.reshape(BATCH, HEADS * VHEAD), w_out, preferred_element_type=jnp.float32)
    return (hidden.astype(jnp.float32) + attn_out).astype(jnp.bfloat16), lat_all, rope_all
```

```python
import functools
import math
import jax
import jax.numpy as jnp
from jax import lax
from jax.experimental import pallas as pl
from jax.experimental.pallas import tpu as pltpu
from jax.sharding import PartitionSpec as P

EPSILON = 1e-6
ROPE_BASE = 50000.0
YARN_MSCALE = 1.0 + 0.1 * math.log(32.0)
MASK_VALUE = -1e30
CHIPS = 4
SUBLANES = 8
LANES = 128
NT_DIMS = (((1,), (1,)), ((), ()))


def rms_norm(values, gain):
    vals32 = values.astype(jnp.float32)
    inv_rms = lax.rsqrt(jnp.mean(vals32 * vals32, axis=-1, keepdims=True) + EPSILON)
    return vals32 * inv_rms * gain.astype(jnp.float32)


def rope_tables(positions, rope_dim):
    half_dim = rope_dim // 2
    inv_freq = ROPE_BASE ** (-jnp.arange(half_dim).astype(jnp.float32) / half_dim)
    angles = positions.astype(jnp.float32)[:, None] * inv_freq[None, :]
    return jnp.cos(angles), jnp.sin(angles)


def rotate_pairs(values, cos_t, sin_t):
    half_dim = values.shape[-1] // 2
    first_half = values[..., :half_dim]
    second_half = values[..., half_dim:]
    return jnp.concatenate([first_half * cos_t - second_half * sin_t, second_half * cos_t + first_half * sin_t], axis=-1)


def project_inputs(hidden, positions, w_dq, gain_q, w_dkv, gain_kv, w_uq, w_uk):
    kv_rank = w_uk.shape[0]
    nope_dim = w_uk.shape[2]
    cos_t, sin_t = rope_tables(positions, w_uq.shape[2] - nope_dim)
    h_q = jnp.dot(hidden, w_dq, preferred_element_type=jnp.float32).astype(jnp.bfloat16)
    c_q = rms_norm(h_q, gain_q).astype(jnp.bfloat16)
    q_full = jnp.einsum('br,rhd->bhd', c_q, w_uq, preferred_element_type=jnp.float32).astype(jnp.bfloat16)
    q_rope = rotate_pairs(q_full[:, :, nope_dim:].astype(jnp.float32), cos_t[:, None, :], sin_t[:, None, :]).astype(jnp.bfloat16)
    q_abs = jnp.einsum('bhn,khn->bhk', q_full[:, :, :nope_dim], w_uk, preferred_element_type=jnp.float32).astype(jnp.bfloat16)
    kv_down = jnp.dot(hidden, w_dkv, preferred_element_type=jnp.float32).astype(jnp.bfloat16)
    lat_new = rms_norm(kv_down[:, :kv_rank], gain_kv).astype(jnp.bfloat16)
    rope_new = rotate_pairs(kv_down[:, kv_rank:].astype(jnp.float32), cos_t, sin_t).astype(jnp.bfloat16)
    return q_abs, q_rope, lat_new, rope_new


def merge_parts(parts, lane):
    groups = len(parts[0]) // 4
    stats = [p[-1] for p in parts]
    out, maxes, dens = [], [], []
    for g in range(groups):
        ms = [jnp.broadcast_to(s[:, 2 * g:2 * g + 1], s.shape) for s in stats]
        ls = [jnp.broadcast_to(s[:, 2 * g + 1:2 * g + 2], s.shape) for s in stats]
        top = functools.reduce(jnp.maximum, ms)
        ws = [jnp.exp(m - top) for m in ms]
        maxes.append(top)
        dens.append(sum(w * l for w, l in zip(ws, ls)))
        for n in range(4):
            out.append(sum(w * p[4 * g + n] for w, p in zip(ws, parts)))
    return out, maxes, dens


def pack_stats(maxes, dens, lane):
    tile = jnp.zeros((SUBLANES, LANES), jnp.float32)
    for g, (m, l) in enumerate(zip(maxes, dens)):
        tile = jnp.where(lane == 2 * g, m, tile)
        tile = jnp.where(lane == 2 * g + 1, l, tile)
    return tile


def attend_kernel(rounds, inner, scale, pos_ref, lat_ref, rope_ref, qa_ref, qr_ref, cn_ref, kn_ref, out_ref,
                  part, peer_in, merged, far_in, relay, dir_in, rel_in,
                  peer_send, far_send, dir_send, rel_send, peer_recv, far_recv, dir_recv, rel_recv):
    t = pl.program_id(0)
    me = lax.axis_index('sp')
    chip, core = me // 2, lax.rem(me, 2)
    owners = lat_ref.shape[1]
    slots = lat_ref.shape[3]
    heads, rank = qa_ref.shape[3], qa_ref.shape[4]
    lane = lax.broadcasted_iota(jnp.int32, (SUBLANES, LANES), 1)
    tiles = part.shape[3]

    def at_chip(index):
        return {'sp': lax.rem(index + CHIPS, CHIPS) * 2 + core}

    def peer_copy(r):
        return pltpu.make_async_remote_copy(
            src_ref=part.at[r, 1 - core], dst_ref=peer_in.at[r], send_sem=peer_send.at[lax.rem(r, 4)], recv_sem=peer_recv.at[r],
            device_id={'sp': chip * 2 + 1 - core}, device_id_type=pl.DeviceIdType.MESH)

    def direction(r):
        return 1 - 2 * lax.rem(r, 2)

    def far_copy(r):
        s = direction(r)
        return pltpu.make_async_remote_copy(
            src_ref=merged.at[r, lax.rem(chip + 2, CHIPS)], dst_ref=far_in.at[r], send_sem=far_send.at[lax.rem(r, 4)],
            recv_sem=far_recv.at[r], device_id=at_chip(chip + s), device_id_type=pl.DeviceIdType.MESH)

    def dir_copy(r):
        s = direction(r)
        return pltpu.make_async_remote_copy(
            src_ref=merged.at[r, lax.rem(chip - s + CHIPS, CHIPS)], dst_ref=dir_in.at[r], send_sem=dir_send.at[lax.rem(r, 4)],
            recv_sem=dir_recv.at[r], device_id=at_chip(chip - s), device_id_type=pl.DeviceIdType.MESH)

    def rel_copy(r):
        s = direction(r)
        return pltpu.make_async_remote_copy(
            src_ref=relay.at[r], dst_ref=rel_in.at[r], send_sem=rel_send.at[lax.rem(r, 4)],
            recv_sem=rel_recv.at[r], device_id=at_chip(chip + s), device_id_type=pl.DeviceIdType.MESH)

    @pl.when(t == 0)
    def _():
        barrier = pltpu.get_barrier_semaphore()
        pl.semaphore_signal(barrier, inc=1, device_id={'sp': chip * 2 + 1 - core}, device_id_type=pl.DeviceIdType.MESH)
        pl.semaphore_signal(barrier, inc=1, device_id=at_chip(chip + 1), device_id_type=pl.DeviceIdType.MESH)
        pl.semaphore_signal(barrier, inc=1, device_id=at_chip(chip - 1), device_id_type=pl.DeviceIdType.MESH)
        pl.semaphore_wait(barrier, 3)

    @pl.when(t < rounds)
    def _():
        base = me * slots
        slot = lax.broadcasted_iota(jnp.int32, (heads, slots), 1)
        scores, news, valid, hits, fresh = [], [], [], [], []
        for j in range(owners):
            row = (t // inner) * (owners * inner) + j * inner + lax.rem(t, inner)
            local = pos_ref[row] - base
            qa, qr = qa_ref[0, j, 0], qr_ref[0, j, 0]
            lat_s = lax.dot_general(qa, lat_ref[0, j, 0], NT_DIMS, preferred_element_type=jnp.float32)
            rope_s = jnp.dot(qr, rope_ref[0, j, 0], preferred_element_type=jnp.float32)
            c_new = cn_ref[pl.ds(row, 1), :]
            k_new = kn_ref[pl.ds(row, 1), :]
            s_new = (jnp.sum(qa.astype(jnp.float32) * c_new, axis=-1, keepdims=True)
                     + jnp.sum(qr.astype(jnp.float32) * k_new, axis=-1, keepdims=True)) * scale
            ok = slot < local
            hit = jnp.full((heads, 1), local, jnp.int32)
            hit = (hit >= 0) & (hit < slots)
            scores.append(jnp.where(ok, (lat_s + rope_s) * scale, MASK_VALUE))
            news.append(jnp.where(hit, s_new, MASK_VALUE))
            valid.append(ok)
            hits.append(hit)
            fresh.append(c_new)
        for j in range(owners):
            top = jnp.maximum(jnp.max(scores[j], axis=-1, keepdims=True), news[j])
            weights = jnp.where(valid[j], jnp.exp(scores[j] - top), 0.0)
            w_new = jnp.where(hits[j], jnp.exp(news[j] - top), 0.0)
            den = jnp.sum(weights, axis=-1, keepdims=True) + w_new
            lat_sum = jnp.dot(weights.astype(jnp.bfloat16), lat_ref[0, j, 0], preferred_element_type=jnp.float32)
            lat_sum = lat_sum + w_new.astype(jnp.bfloat16).astype(jnp.float32) * fresh[j]
            for g in range(heads // SUBLANES):
                for n in range(rank // LANES):
                    part[t, j % 2, j // 2, 4 * g + n] = lat_sum[SUBLANES * g:SUBLANES * (g + 1), LANES * n:LANES * (n + 1)]
            split = [slice(SUBLANES * g, SUBLANES * (g + 1)) for g in range(heads // SUBLANES)]
            part[t, j % 2, j // 2, tiles - 1] = pack_stats([top[g] for g in split], [den[g] for g in split], lane)

    @pl.when((t >= 1) & (t < rounds + 1))
    def _():
        r = t - 1
        peer_copy(r).wait()
        for d in range(CHIPS):
            mine = [part[r, core, d, n] for n in range(tiles)]
            theirs = [peer_in[r, d, n] for n in range(tiles)]
            out, maxes, dens = merge_parts([mine, theirs], lane)
            for n in range(tiles - 1):
                merged[r, d, n] = out[n]
            merged[r, d, tiles - 1] = pack_stats(maxes, dens, lane)

    @pl.when(t < rounds)
    def _():
        peer_copy(t).start()

    @pl.when((t >= 3) & (t < rounds + 3))
    def _():
        r = t - 3
        far_copy(r).wait()
        d = lax.rem(chip + direction(r) + CHIPS, CHIPS)
        mine = [merged[r, d, n] for n in range(tiles)]
        theirs = [far_in[r, n] for n in range(tiles)]
        out, maxes, dens = merge_parts([mine, theirs], lane)
        for n in range(tiles - 1):
            relay[r, n] = out[n]
        relay[r, tiles - 1] = pack_stats(maxes, dens, lane)

    @pl.when((t >= 1) & (t < rounds + 1))
    def _():
        far_copy(t - 1).start()
        dir_copy(t - 1).start()

    @pl.when(t >= 5)
    def _():
        r = t - 5
        dir_copy(r).wait()
        rel_copy(r).wait()
        parts = [[merged[r, chip, n] for n in range(tiles)], [dir_in[r, n] for n in range(tiles)], [rel_in[r, n] for n in range(tiles)]]
        out, _, dens = merge_parts(parts, lane)
        rows = [jnp.concatenate([out[4 * g + n] / dens[g] for n in range(rank // LANES)], axis=-1) for g in range(heads // SUBLANES)]
        out_ref[r] = jnp.concatenate(rows, axis=0).astype(jnp.bfloat16)

    @pl.when((t >= 3) & (t < rounds + 3))
    def _():
        rel_copy(t - 3).start()


def attend_shards(positions, lat, rope_t, q_abs, q_rope, lat_new, rope_new, scale, n_tp, n_sp):
    rows, slots, rank = lat.shape
    heads, rope_dim = q_rope.shape[1:]
    inner = rows // (n_tp * n_sp)
    rounds = rows // n_sp
    drain = 5
    view = lambda a: a.reshape((n_tp, n_sp, inner) + a.shape[1:])

    def block(*dims):
        def index(t, pos):
            r = jnp.minimum(t, rounds - 1)
            return (r // inner, 0, lax.rem(r, inner)) + (0,) * len(dims)
        return pl.BlockSpec((1, n_sp, 1) + dims, index)

    whole = lambda a: pl.BlockSpec(a.shape, lambda t, pos: (0,) * a.ndim)
    tiles = (heads // SUBLANES) * (rank // LANES) + 1
    tile_set = (tiles, SUBLANES, LANES)
    vmem = lambda *lead: pltpu.VMEM(lead + tile_set, jnp.float32)
    sems = lambda n: pltpu.SemaphoreType.DMA((n,))
    lat_new, rope_new = lat_new.astype(jnp.float32), rope_new.astype(jnp.float32)
    return pl.pallas_call(
        functools.partial(attend_kernel, rounds, inner, scale),
        grid_spec=pltpu.PrefetchScalarGridSpec(
            num_scalar_prefetch=1,
            grid=(rounds + drain,),
            in_specs=[block(slots, rank), block(rope_dim, slots), block(heads, rank), block(heads, rope_dim), whole(lat_new), whole(rope_new)],
            out_specs=pl.BlockSpec((rounds, heads, rank), lambda t, pos: (0, 0, 0)),
            scratch_shapes=[
                vmem(rounds, 2, CHIPS), vmem(rounds, CHIPS), vmem(rounds, CHIPS), vmem(rounds), vmem(rounds), vmem(rounds), vmem(rounds),
                sems(4), sems(4), sems(4), sems(4), sems(rounds), sems(rounds), sems(rounds), sems(rounds),
            ],
        ),
        out_shape=jax.ShapeDtypeStruct((rounds, heads, rank), jnp.bfloat16),
        compiler_params=pltpu.CompilerParams(collective_id=0, has_side_effects=True, vmem_limit_bytes=48 * 2 ** 20, dimension_semantics=('arbitrary',)),
        name='attend',
    )(positions, view(lat), view(rope_t), view(q_abs), view(q_rope), lat_new, rope_new)


def solution(mesh):
    row_spec = P('dp', None)
    cache_spec = P('dp', 'sp', None)
    head_spec = P(None, 'tp', None)
    in_specs = (row_spec, cache_spec, cache_spec, P('dp'), P(), P(), P(), P(), head_spec, head_spec, head_spec, P('tp', None))
    out_specs = (row_spec, cache_spec, cache_spec)
    n_tp, n_sp = mesh.shape['tp'], mesh.shape['sp']

    def local_step(hidden, lat_cache, rope_cache, positions, w_dq, gain_q, w_dkv, gain_kv, w_uq, w_uk, w_uv, w_out):
        seq_local = lat_cache.shape[1]
        score_scale = YARN_MSCALE ** 2 / math.sqrt(w_uq.shape[2])
        q_abs, q_rope, lat_new, rope_new = project_inputs(hidden, positions, w_dq, gain_q, w_dkv, gain_kv, w_uq, w_uk)
        rope_t = jnp.swapaxes(rope_cache, 1, 2)
        o_lat = attend_shards(positions, lat_cache, rope_t, q_abs, q_rope, lat_new, rope_new, score_scale, n_tp, n_sp)
        o_heads = jnp.einsum('bhk,khv->bhv', o_lat, w_uv, preferred_element_type=jnp.float32).astype(jnp.bfloat16)
        attn_part = jnp.dot(o_heads.reshape(o_heads.shape[0], -1), w_out, preferred_element_type=jnp.float32)
        attn_rows = lax.psum_scatter(attn_part, 'tp', scatter_dimension=0, tiled=True)
        attn_out = lax.all_gather(attn_rows, ('tp', 'sp'), axis=0, tiled=True)
        slot_ids = lax.axis_index('sp') * seq_local + jnp.arange(seq_local)
        slot_hit = (slot_ids[None, :] == positions[:, None])[:, :, None]
        lat_all = jnp.where(slot_hit, lat_new[:, None, :], lat_cache)
        rope_all = jnp.where(slot_hit, rope_new[:, None, :], rope_cache)
        return (hidden.astype(jnp.float32) + attn_out).astype(jnp.bfloat16), lat_all, rope_all

    return jax.shard_map(local_step, mesh=mesh, in_specs=in_specs, out_specs=out_specs, check_vma=False)
```

```python
import functools
import math
import jax
import jax.numpy as jnp
from jax import lax
from jax.experimental import pallas as pl
from jax.experimental.pallas import tpu as pltpu
from jax.sharding import PartitionSpec as P

EPSILON = 1e-6
ROPE_BASE = 50000.0
YARN_MSCALE = 1.0 + 0.1 * math.log(32.0)
MASK_VALUE = -1e30
LAT_DEPTH = 5
CHIPS = 4
SUBLANES = 8
LANES = 128
NT_DIMS = (((1,), (1,)), ((), ()))


def rms_norm(values, gain):
    vals32 = values.astype(jnp.float32)
    inv_rms = lax.rsqrt(jnp.mean(vals32 * vals32, axis=-1, keepdims=True) + EPSILON)
    return vals32 * inv_rms * gain.astype(jnp.float32)


def rope_tables(positions, rope_dim):
    half_dim = rope_dim // 2
    inv_freq = ROPE_BASE ** (-jnp.arange(half_dim).astype(jnp.float32) / half_dim)
    angles = positions.astype(jnp.float32)[:, None] * inv_freq[None, :]
    return jnp.cos(angles), jnp.sin(angles)


def rotate_pairs(values, cos_t, sin_t):
    half_dim = values.shape[-1] // 2
    first_half = values[..., :half_dim]
    second_half = values[..., half_dim:]
    return jnp.concatenate([first_half * cos_t - second_half * sin_t, second_half * cos_t + first_half * sin_t], axis=-1)


def project_inputs(hidden, positions, w_dq, gain_q, w_dkv, gain_kv, w_uq, w_uk):
    kv_rank = w_uk.shape[0]
    nope_dim = w_uk.shape[2]
    cos_t, sin_t = rope_tables(positions, w_uq.shape[2] - nope_dim)
    h_q = jnp.dot(hidden, w_dq, preferred_element_type=jnp.float32).astype(jnp.bfloat16)
    c_q = rms_norm(h_q, gain_q).astype(jnp.bfloat16)
    q_full = jnp.einsum('br,rhd->bhd', c_q, w_uq, preferred_element_type=jnp.float32).astype(jnp.bfloat16)
    q_rope = rotate_pairs(q_full[:, :, nope_dim:].astype(jnp.float32), cos_t[:, None, :], sin_t[:, None, :]).astype(jnp.bfloat16)
    q_abs = jnp.einsum('bhn,khn->bhk', q_full[:, :, :nope_dim], w_uk, preferred_element_type=jnp.float32).astype(jnp.bfloat16)
    kv_down = jnp.dot(hidden, w_dkv, preferred_element_type=jnp.float32).astype(jnp.bfloat16)
    lat_new = rms_norm(kv_down[:, :kv_rank], gain_kv).astype(jnp.bfloat16)
    rope_new = rotate_pairs(kv_down[:, kv_rank:].astype(jnp.float32), cos_t, sin_t).astype(jnp.bfloat16)
    return q_abs, q_rope, lat_new, rope_new


def merge_parts(parts, lane):
    groups = len(parts[0]) // 4
    stats = [p[-1] for p in parts]
    out, maxes, dens = [], [], []
    for g in range(groups):
        ms = [jnp.broadcast_to(s[:, 2 * g:2 * g + 1], s.shape) for s in stats]
        ls = [jnp.broadcast_to(s[:, 2 * g + 1:2 * g + 2], s.shape) for s in stats]
        top = functools.reduce(jnp.maximum, ms)
        ws = [jnp.exp(m - top) for m in ms]
        maxes.append(top)
        dens.append(sum(w * l for w, l in zip(ws, ls)))
        for n in range(4):
            out.append(sum(w * p[4 * g + n] for w, p in zip(ws, parts)))
    return out, maxes, dens


def pack_stats(maxes, dens, lane):
    tile = jnp.zeros((SUBLANES, LANES), jnp.float32)
    for g, (m, l) in enumerate(zip(maxes, dens)):
        tile = jnp.where(lane == 2 * g, m, tile)
        tile = jnp.where(lane == 2 * g + 1, l, tile)
    return tile


def attend_kernel(rounds, inner, lags, scale, pos_ref, qa_ref, qr_ref, cn_ref, kn_ref, lat_ref, rope_ref, out_ref,
                  lat_buf, rope_buf, probs, new_probs, part, peer_in, merged, far_in, relay, dir_in, rel_in,
                  lat_sem, rope_sem, peer_send, far_send, dir_send, rel_send, peer_recv, far_recv, dir_recv, rel_recv):
    me = lax.axis_index('sp')
    chip, core = me // 2, lax.rem(me, 2)
    owners = lat_ref.shape[1]
    slots = lat_ref.shape[3]
    heads, rank = qa_ref.shape[3], qa_ref.shape[4]
    lane = lax.broadcasted_iota(jnp.int32, (SUBLANES, LANES), 1)
    tiles = part.shape[3]
    depth = lat_buf.shape[0]
    split = [slice(SUBLANES * g, SUBLANES * (g + 1)) for g in range(heads // SUBLANES)]
    lag_peer, lag_far, lag_last = lags

    def at_chip(index):
        return {'sp': lax.rem(index + CHIPS, CHIPS) * 2 + core}

    def direction(r):
        return 1 - 2 * lax.rem(r, 2)

    def remote(src, dst, send, recv, r, target):
        return pltpu.make_async_remote_copy(
            src_ref=src, dst_ref=dst.at[r], send_sem=send.at[lax.rem(r, send.shape[0])], recv_sem=recv.at[r],
            device_id=target, device_id_type=pl.DeviceIdType.MESH)

    def peer_copy(r):
        return remote(part.at[r, 1 - core], peer_in, peer_send, peer_recv, r, {'sp': chip * 2 + 1 - core})

    def far_copy(r):
        return remote(merged.at[r, lax.rem(chip + 2, CHIPS)], far_in, far_send, far_recv, r, at_chip(chip + direction(r)))

    def dir_copy(r):
        source = lax.rem(chip - direction(r) + CHIPS, CHIPS)
        return remote(merged.at[r, source], dir_in, dir_send, dir_recv, r, at_chip(chip - direction(r)))

    def rel_copy(r):
        return remote(relay.at[r], rel_in, rel_send, rel_recv, r, at_chip(chip + direction(r)))

    def lat_copy(r):
        slot = lax.rem(r, depth)
        return pltpu.make_async_copy(lat_ref.at[r // inner, :, lax.rem(r, inner)], lat_buf.at[slot], lat_sem.at[slot])

    def rope_copy(r):
        slot = lax.rem(r, depth)
        return pltpu.make_async_copy(rope_ref.at[r // inner, :, lax.rem(r, inner)], rope_buf.at[slot], rope_sem.at[slot])

    def fetch(r):
        lat_copy(r).start()
        rope_copy(r).start()

    def arrive(r):
        lat_copy(r).wait()
        rope_copy(r).wait()

    def row_of(r, j):
        return (r // inner) * (owners * inner) + j * inner + lax.rem(r, inner)

    def score(r, j):
        buf = lax.rem(r, depth)
        lat_s = lax.dot_general(qa_ref[r // inner, j, lax.rem(r, inner)], lat_buf[buf, j], NT_DIMS, preferred_element_type=jnp.float32)
        rope_s = jnp.dot(qr_ref[r // inner, j, lax.rem(r, inner)], rope_buf[buf, j], preferred_element_type=jnp.float32)
        return lat_s + rope_s

    def soften(r, j, raw):
        row = row_of(r, j)
        local = pos_ref[row] - me * slots
        slot = lax.broadcasted_iota(jnp.int32, (heads, slots), 1)
        qa, qr = qa_ref[r // inner, j, lax.rem(r, inner)], qr_ref[r // inner, j, lax.rem(r, inner)]
        s_new = (jnp.sum(qa.astype(jnp.float32) * cn_ref[pl.ds(row, 1), :], axis=-1, keepdims=True)
                 + jnp.sum(qr.astype(jnp.float32) * kn_ref[pl.ds(row, 1), :], axis=-1, keepdims=True)) * scale
        ok = slot < local
        hit = jnp.full((heads, 1), local, jnp.int32)
        hit = (hit >= 0) & (hit < slots)
        scores = jnp.where(ok, raw * scale, MASK_VALUE)
        s_new = jnp.where(hit, s_new, MASK_VALUE)
        top = jnp.maximum(jnp.max(scores, axis=-1, keepdims=True), s_new)
        weights = jnp.where(ok, jnp.exp(scores - top), 0.0)
        w_new = jnp.where(hit, jnp.exp(s_new - top), 0.0)
        den = jnp.sum(weights, axis=-1, keepdims=True) + w_new
        stats = pack_stats([top[g] for g in split], [den[g] for g in split], lane)
        return weights.astype(jnp.bfloat16), jnp.broadcast_to(w_new.astype(jnp.bfloat16).astype(jnp.float32), (heads, LANES)), stats

    def keep(r, soft):
        half = lax.rem(r, 2)
        for j, (weights, w_new, stats) in enumerate(soft):
            probs[half, j] = weights
            new_probs[half, j] = w_new
            part[r, j % 2, j // 2, tiles - 1] = stats

    def weigh(r, j):
        buf, half = lax.rem(r, depth), lax.rem(r, 2)
        lat_sum = jnp.dot(probs[half, j], lat_buf[buf, j], preferred_element_type=jnp.float32)
        w_new, c_new = new_probs[half, j], cn_ref[pl.ds(row_of(r, j), 1), :]
        for g in range(heads // SUBLANES):
            for n in range(rank // LANES):
                cols = slice(LANES * n, LANES * (n + 1))
                part[r, j % 2, j // 2, 4 * g + n] = lat_sum[split[g], cols] + w_new[split[g]] * c_new[:, cols]

    def put(dst, index, out, maxes, dens):
        for n in range(tiles - 1):
            dst[(*index, n)] = out[n]
        dst[(*index, tiles - 1)] = pack_stats(maxes, dens, lane)

    def merge_peer(r):
        for d in range(CHIPS):
            put(merged, (r, d), *merge_parts([[part[r, core, d, n] for n in range(tiles)], [peer_in[r, d, n] for n in range(tiles)]], lane))

    def merge_far(r):
        d = lax.rem(chip + direction(r) + CHIPS, CHIPS)
        put(relay, (r,), *merge_parts([[merged[r, d, n] for n in range(tiles)], [far_in[r, n] for n in range(tiles)]], lane))

    def merge_last(r):
        parts = [[merged[r, chip, n] for n in range(tiles)], [dir_in[r, n] for n in range(tiles)], [rel_in[r, n] for n in range(tiles)]]
        out, _, dens = merge_parts(parts, lane)
        rows = [jnp.concatenate([out[4 * g + n] / dens[g] for n in range(rank // LANES)], axis=-1) for g in range(heads // SUBLANES)]
        out_ref[r] = jnp.concatenate(rows, axis=0).astype(jnp.bfloat16)

    def start_sends(r):
        far_copy(r).start()
        dir_copy(r).start()

    def wait_last(r):
        dir_copy(r).wait()
        rel_copy(r).wait()

    for r in range(depth - 2):
        fetch(r)
    barrier = pltpu.get_barrier_semaphore()
    pl.semaphore_signal(barrier, inc=1, device_id={'sp': chip * 2 + 1 - core}, device_id_type=pl.DeviceIdType.MESH)
    pl.semaphore_signal(barrier, inc=1, device_id=at_chip(chip + 1), device_id_type=pl.DeviceIdType.MESH)
    pl.semaphore_signal(barrier, inc=1, device_id=at_chip(chip - 1), device_id_type=pl.DeviceIdType.MESH)
    pl.semaphore_wait(barrier, 3)

    def fetch_ahead(t):
        @pl.when(t < rounds - (depth - 2))
        def _():
            fetch(t + depth - 2)

    def edge_step(t, scoring):
        def stage(lag, *actions):
            @pl.when((t >= lag) & (t < rounds + lag))
            def _():
                for action in actions:
                    action(t - lag)

        if scoring:
            fetch_ahead(t)
            arrive(t)
            keep(t, [soften(t, j, score(t, j)) for j in range(owners)])
        stage(1, lambda r: [weigh(r, j) for j in range(owners)])
        stage(lag_peer, lambda r: peer_copy(r).wait(), merge_peer, start_sends)
        stage(lag_far, lambda r: far_copy(r).wait(), merge_far, lambda r: rel_copy(r).start())
        stage(lag_last, wait_last, merge_last)
        stage(1, lambda r: peer_copy(r).start())

    @pl.loop(0, lag_last)
    def _(t):
        edge_step(t, True)

    @pl.loop(lag_last, rounds)
    def _(t):
        fetch_ahead(t)
        arrive(t)
        peer_copy(t - lag_peer).wait()
        far_copy(t - lag_far).wait()
        wait_last(t - lag_last)
        merge_last(t - lag_last)
        merge_far(t - lag_far)
        merge_peer(t - lag_peer)
        raw = [score(t, j) for j in range(owners)]
        for j in range(owners):
            weigh(t - 1, j)
        keep(t, [soften(t, j, raw[j]) for j in range(owners)])
        start_sends(t - lag_peer)
        rel_copy(t - lag_far).start()
        peer_copy(t - 1).start()

    @pl.loop(rounds, rounds + lag_last)
    def _(t):
        edge_step(t, False)


def attend_shards(positions, lat, rope_t, q_abs, q_rope, lat_new, rope_new, scale, n_tp, n_sp):
    rows, slots, rank = lat.shape
    heads, rope_dim = q_rope.shape[1:]
    inner = rows // (n_tp * n_sp)
    rounds = rows // n_sp
    lags = (3, 7, 11)
    view = lambda a: a.reshape((n_tp, n_sp, inner) + a.shape[1:])

    tiles = (heads // SUBLANES) * (rank // LANES) + 1
    tile_set = (tiles, SUBLANES, LANES)
    vmem = lambda *lead: pltpu.VMEM(lead + tile_set, jnp.float32)
    sems = lambda n: pltpu.SemaphoreType.DMA((n,))
    lat_new, rope_new = lat_new.astype(jnp.float32), rope_new.astype(jnp.float32)
    return pl.pallas_call(
        functools.partial(attend_kernel, rounds, inner, lags, scale),
        in_specs=[pl.BlockSpec(memory_space=pltpu.SMEM)] + [pl.BlockSpec(memory_space=pltpu.VMEM)] * 4 + [pl.BlockSpec(memory_space=pl.ANY)] * 2,
        out_specs=pl.BlockSpec(memory_space=pltpu.VMEM),
        scratch_shapes=[
            pltpu.VMEM((LAT_DEPTH, n_sp, slots, rank), lat.dtype), pltpu.VMEM((LAT_DEPTH, n_sp, rope_dim, slots), rope_t.dtype),
            pltpu.VMEM((2, n_sp, heads, slots), jnp.bfloat16), pltpu.VMEM((2, n_sp, heads, LANES), jnp.float32),
            vmem(rounds, 2, CHIPS), vmem(rounds, CHIPS), vmem(rounds, CHIPS), vmem(rounds), vmem(rounds), vmem(rounds), vmem(rounds),
            sems(LAT_DEPTH), sems(LAT_DEPTH), sems(8), sems(8), sems(8), sems(8), sems(rounds), sems(rounds), sems(rounds), sems(rounds),
        ],
        out_shape=jax.ShapeDtypeStruct((rounds, heads, rank), jnp.bfloat16),
        compiler_params=pltpu.CompilerParams(collective_id=0, has_side_effects=True, vmem_limit_bytes=48 * 2 ** 20),
        name='attend',
    )(positions, view(q_abs), view(q_rope), lat_new, rope_new, view(lat), view(rope_t))


def project_kernel(chunks, cols, o_ref, w_ref, out_ref, w_buf, part, far_in, relay, dir_in, rel_in,
                   w_sem, far_send, dir_send, rel_send, far_recv, dir_recv, rel_recv):
    ring = CHIPS
    me = lax.axis_index('tp')
    depth = w_buf.shape[0]
    lag_far, lag_last = 2, 4

    def device(index):
        return {'tp': lax.rem(index + ring, ring)}

    def direction(n):
        return 1 - 2 * lax.rem(n, 2)

    def rows(index):
        return pl.ds(pl.multiple_of(lax.rem(index + ring, ring) * SUBLANES, SUBLANES), SUBLANES)

    def columns(n):
        return pl.ds(pl.multiple_of(n * cols, cols), cols)

    def remote(src, dst, send, recv, n, target):
        return pltpu.make_async_remote_copy(src_ref=src, dst_ref=dst.at[n], send_sem=send.at[n], recv_sem=recv.at[n],
                                            device_id=target, device_id_type=pl.DeviceIdType.MESH)

    def far_copy(n):
        return remote(part.at[n, rows(me + 2)], far_in, far_send, far_recv, n, device(me + direction(n)))

    def dir_copy(n):
        return remote(part.at[n, rows(me - direction(n))], dir_in, dir_send, dir_recv, n, device(me - direction(n)))

    def rel_copy(n):
        return remote(relay.at[n], rel_in, rel_send, rel_recv, n, device(me + direction(n)))

    def fetch(n):
        slot = lax.rem(n, depth)
        return pltpu.make_async_copy(w_ref.at[:, columns(n)], w_buf.at[slot], w_sem.at[slot])

    for n in range(depth - 1):
        fetch(n).start()
    barrier = pltpu.get_barrier_semaphore()
    pl.semaphore_signal(barrier, inc=1, device_id=device(me + 1), device_id_type=pl.DeviceIdType.MESH)
    pl.semaphore_signal(barrier, inc=1, device_id=device(me - 1), device_id_type=pl.DeviceIdType.MESH)
    pl.semaphore_wait(barrier, 2)

    @pl.loop(0, chunks + lag_last)
    def _(t):
        @pl.when(t < chunks - (depth - 1))
        def _():
            fetch(t + depth - 1).start()

        @pl.when(t < chunks)
        def _():
            fetch(t).wait()
            part[t] = jnp.dot(o_ref[...], w_buf[lax.rem(t, depth)], preferred_element_type=jnp.float32)

        @pl.when((t >= lag_last) & (t < chunks + lag_last))
        def _():
            n = t - lag_last
            dir_copy(n).wait()
            rel_copy(n).wait()
            out_ref[:, columns(n)] = part[n, rows(me)] + dir_in[n] + rel_in[n]

        @pl.when((t >= lag_far) & (t < chunks + lag_far))
        def _():
            n = t - lag_far
            far_copy(n).wait()
            relay[n] = part[n, rows(me + direction(n))] + far_in[n]

        @pl.when(t < chunks)
        def _():
            far_copy(t).start()
            dir_copy(t).start()

        @pl.when((t >= lag_far) & (t < chunks + lag_far))
        def _():
            rel_copy(t - lag_far).start()


def project_out(o_rows, w_out):
    rows, depth = o_rows.shape
    width = w_out.shape[1]
    cols = 1024
    chunks = width // cols
    block = lambda *lead: pltpu.VMEM(lead, jnp.float32)
    sems = pltpu.SemaphoreType.DMA((chunks,))
    return pl.pallas_call(
        functools.partial(project_kernel, chunks, cols),
        in_specs=[pl.BlockSpec(memory_space=pltpu.VMEM), pl.BlockSpec(memory_space=pl.ANY)],
        out_specs=pl.BlockSpec(memory_space=pltpu.VMEM),
        out_shape=jax.ShapeDtypeStruct((SUBLANES, width), jnp.float32),
        scratch_shapes=[
            pltpu.VMEM((4, depth, cols), w_out.dtype), block(chunks, rows, cols),
            block(chunks, SUBLANES, cols), block(chunks, SUBLANES, cols), block(chunks, SUBLANES, cols), block(chunks, SUBLANES, cols),
            pltpu.SemaphoreType.DMA((4,)), sems, sems, sems, sems, sems, sems,
        ],
        compiler_params=pltpu.CompilerParams(collective_id=1, has_side_effects=True, vmem_limit_bytes=28 * 2 ** 20),
        cost_estimate=pl.CostEstimate(flops=2 * rows * depth * width, bytes_accessed=2 * depth * width, transcendentals=0),
        name='project_out',
    )(o_rows, w_out)


def update_kernel(group, pos_ref, lat_ref, rope_ref, new_ref, col_ref, after_ref, lat_out, rope_out):
    first = pl.program_id(0) * group
    slots, rank = lat_ref.shape[1:]
    lat_out[...] = lat_ref[...]
    slot_row = lax.broadcasted_iota(jnp.int32, (16, rank), 0)
    slot_col = lax.broadcasted_iota(jnp.int32, rope_ref.shape[1:], 1)
    for j in range(group):
        local = pos_ref[first + j]
        start = pl.multiple_of(jnp.clip(local, 0, slots - 1) // 16 * 16, 16)
        window = lat_ref[j, pl.ds(start, 16), :].astype(jnp.float32)
        window = jnp.where(slot_row == local - start, new_ref[j:j + 1, :], window)
        lat_out[j, pl.ds(start, 16), :] = window.astype(lat_out.dtype)
        rope = jnp.where(slot_col == local, col_ref[0, :, j:j + 1], rope_ref[j].astype(jnp.float32))
        rope_out[j] = rope.astype(rope_out.dtype)


def update_caches(local_pos, lat, rope_t, lat_new, rope_new, after):
    rows, slots, rank = lat.shape
    rope_dim = rope_t.shape[1]
    group = 8
    cols = rope_new.reshape(rows // group, group, rope_dim).swapaxes(1, 2)
    lead = lambda *dims: pl.BlockSpec(dims, lambda i, pos: (i,) + (0,) * (len(dims) - 1))
    return pl.pallas_call(
        functools.partial(update_kernel, group),
        grid_spec=pltpu.PrefetchScalarGridSpec(
            num_scalar_prefetch=1,
            grid=(rows // group,),
            in_specs=[lead(group, slots, rank), lead(group, rope_dim, slots), lead(group, rank), lead(1, rope_dim, group), pl.BlockSpec(memory_space=pl.ANY)],
            out_specs=[lead(group, slots, rank), lead(group, rope_dim, slots)],
        ),
        out_shape=[jax.ShapeDtypeStruct(lat.shape, lat.dtype), jax.ShapeDtypeStruct(rope_t.shape, rope_t.dtype)],
        compiler_params=pltpu.CompilerParams(vmem_limit_bytes=60 * 2 ** 20, dimension_semantics=('arbitrary',)),
        cost_estimate=pl.CostEstimate(flops=50_000_000_000, bytes_accessed=4 * lat.size + 4 * rope_t.size, transcendentals=0),
        name='update_caches',
    )(local_pos, lat, rope_t, lat_new, cols, after)


def solution(mesh):
    row_spec = P('dp', None)
    cache_spec = P('dp', 'sp', None)
    head_spec = P(None, 'tp', None)
    in_specs = (row_spec, cache_spec, cache_spec, P('dp'), P(), P(), P(), P(), head_spec, head_spec, head_spec, P('tp', None))
    out_specs = (row_spec, cache_spec, cache_spec)
    n_tp, n_sp = mesh.shape['tp'], mesh.shape['sp']

    def local_step(hidden, lat_cache, rope_cache, positions, w_dq, gain_q, w_dkv, gain_kv, w_uq, w_uk, w_uv, w_out):
        seq_local = lat_cache.shape[1]
        score_scale = YARN_MSCALE ** 2 / math.sqrt(w_uq.shape[2])
        q_abs, q_rope, lat_new, rope_new = project_inputs(hidden, positions, w_dq, gain_q, w_dkv, gain_kv, w_uq, w_uk)
        rope_t = jnp.swapaxes(rope_cache, 1, 2)
        o_lat = attend_shards(positions, lat_cache, rope_t, q_abs, q_rope, lat_new, rope_new, score_scale, n_tp, n_sp)
        o_heads = jnp.einsum('bhk,khv->bhv', o_lat, w_uv, preferred_element_type=jnp.float32).astype(jnp.bfloat16)
        attn_rows = project_out(o_heads.reshape(o_heads.shape[0], -1), w_out)
        attn_out = lax.all_gather(attn_rows, ('tp', 'sp'), axis=0, tiled=True)
        local_pos = positions - lax.axis_index('sp') * seq_local
        lat_all, rope_all = update_caches(local_pos, lat_cache, rope_t, lat_new.astype(jnp.float32), rope_new.astype(jnp.float32), attn_rows)
        return (hidden.astype(jnp.float32) + attn_out).astype(jnp.bfloat16), lat_all, jnp.swapaxes(rope_all, 1, 2)

    return jax.shard_map(local_step, mesh=mesh, in_specs=in_specs, out_specs=out_specs, check_vma=False)
```

```python
import functools
import math
import jax
import jax.numpy as jnp
from jax import lax
from jax.experimental import pallas as pl
from jax.experimental.pallas import tpu as pltpu
from jax.sharding import PartitionSpec as P

EPSILON = 1e-6
ROPE_BASE = 50000.0
YARN_MSCALE = 1.0 + 0.1 * math.log(32.0)
MASK_VALUE = -1e30
LAT_DEPTH = 5
CHIPS = 4
SUBLANES = 8
LANES = 128
NT_DIMS = (((1,), (1,)), ((), ()))


def rms_norm(values, gain):
    vals32 = values.astype(jnp.float32)
    inv_rms = lax.rsqrt(jnp.mean(vals32 * vals32, axis=-1, keepdims=True) + EPSILON)
    return vals32 * inv_rms * gain.astype(jnp.float32)


def rope_tables(positions, rope_dim):
    half_dim = rope_dim // 2
    inv_freq = ROPE_BASE ** (-jnp.arange(half_dim).astype(jnp.float32) / half_dim)
    angles = positions.astype(jnp.float32)[:, None] * inv_freq[None, :]
    return jnp.cos(angles), jnp.sin(angles)


def rotate_pairs(values, cos_t, sin_t):
    half_dim = values.shape[-1] // 2
    first_half = values[..., :half_dim]
    second_half = values[..., half_dim:]
    return jnp.concatenate([first_half * cos_t - second_half * sin_t, second_half * cos_t + first_half * sin_t], axis=-1)


def project_inputs(hidden, positions, w_dq, gain_q, w_dkv, gain_kv, w_uq, w_uk):
    nope_dim = w_uk.shape[2]
    cos_t, sin_t = rope_tables(positions, w_uq.shape[2] - nope_dim)
    c_q, lat_new, k_rope = project_down(hidden, w_dq, gain_q, w_dkv, gain_kv)
    q_full = jnp.einsum('br,rhd->bhd', c_q, w_uq, preferred_element_type=jnp.float32).astype(jnp.bfloat16)
    q_rope = rotate_pairs(q_full[:, :, nope_dim:].astype(jnp.float32), cos_t[:, None, :], sin_t[:, None, :]).astype(jnp.bfloat16)
    q_rope = jnp.transpose(lax.optimization_barrier(jnp.transpose(q_rope, (1, 2, 0))), (2, 0, 1))
    q_abs = jnp.einsum('bhn,khn->bhk', q_full[:, :, :nope_dim], w_uk, preferred_element_type=jnp.float32).astype(jnp.bfloat16)
    rope_new = rotate_pairs(k_rope, cos_t, sin_t).astype(jnp.bfloat16)
    return q_abs, q_rope, lat_new, rope_new


def merge_parts(parts, lane):
    groups = len(parts[0]) // 4
    stats = [p[-1] for p in parts]
    out, maxes, dens = [], [], []
    for g in range(groups):
        ms = [jnp.broadcast_to(s[:, 2 * g:2 * g + 1], s.shape) for s in stats]
        ls = [jnp.broadcast_to(s[:, 2 * g + 1:2 * g + 2], s.shape) for s in stats]
        top = functools.reduce(jnp.maximum, ms)
        ws = [jnp.exp(m - top) for m in ms]
        maxes.append(top)
        dens.append(sum(w * l for w, l in zip(ws, ls)))
        for n in range(4):
            out.append(sum(w * p[4 * g + n] for w, p in zip(ws, parts)))
    return out, maxes, dens


def pack_stats(maxes, dens, lane):
    tile = jnp.zeros((SUBLANES, LANES), jnp.float32)
    for g, (m, l) in enumerate(zip(maxes, dens)):
        tile = jnp.where(lane == 2 * g, m, tile)
        tile = jnp.where(lane == 2 * g + 1, l, tile)
    return tile


def attend_kernel(rounds, inner, lags, scale, pos_ref, qa_ref, qr_ref, cn_ref, kn_ref, lat_ref, rope_ref, out_ref,
                  lat_buf, rope_buf, probs, new_probs, part, peer_in, merged, far_in, relay, dir_in, rel_in,
                  lat_sem, rope_sem, peer_send, far_send, dir_send, rel_send, peer_recv, far_recv, dir_recv, rel_recv):
    me = lax.axis_index('sp')
    chip, core = me // 2, lax.rem(me, 2)
    owners = lat_ref.shape[1]
    slots = lat_ref.shape[3]
    heads, rank = qa_ref.shape[3], qa_ref.shape[4]
    lane = lax.broadcasted_iota(jnp.int32, (SUBLANES, LANES), 1)
    tiles = part.shape[3]
    depth = lat_buf.shape[0]
    split = [slice(SUBLANES * g, SUBLANES * (g + 1)) for g in range(heads // SUBLANES)]
    lag_peer, lag_far, lag_last = lags

    def at_chip(index):
        return {'sp': lax.rem(index + CHIPS, CHIPS) * 2 + core}

    def direction(r):
        return 1 - 2 * lax.rem(r, 2)

    def remote(src, dst, send, recv, r, target):
        return pltpu.make_async_remote_copy(
            src_ref=src, dst_ref=dst.at[r], send_sem=send.at[lax.rem(r, send.shape[0])], recv_sem=recv.at[r],
            device_id=target, device_id_type=pl.DeviceIdType.MESH)

    def peer_copy(r):
        return remote(part.at[r, 1 - core], peer_in, peer_send, peer_recv, r, {'sp': chip * 2 + 1 - core})

    def far_copy(r):
        return remote(merged.at[r, lax.rem(chip + 2, CHIPS)], far_in, far_send, far_recv, r, at_chip(chip + direction(r)))

    def dir_copy(r):
        source = lax.rem(chip - direction(r) + CHIPS, CHIPS)
        return remote(merged.at[r, source], dir_in, dir_send, dir_recv, r, at_chip(chip - direction(r)))

    def rel_copy(r):
        return remote(relay.at[r], rel_in, rel_send, rel_recv, r, at_chip(chip + direction(r)))

    def lat_copy(r):
        slot = lax.rem(r, depth)
        return pltpu.make_async_copy(lat_ref.at[r // inner, :, lax.rem(r, inner)], lat_buf.at[slot], lat_sem.at[slot])

    def rope_copy(r):
        slot = lax.rem(r, depth)
        return pltpu.make_async_copy(rope_ref.at[r // inner, :, lax.rem(r, inner)], rope_buf.at[slot], rope_sem.at[slot])

    def fetch(r):
        lat_copy(r).start()
        rope_copy(r).start()

    def arrive(r):
        lat_copy(r).wait()
        rope_copy(r).wait()

    def row_of(r, j):
        return (r // inner) * (owners * inner) + j * inner + lax.rem(r, inner)

    def score(r, j):
        buf = lax.rem(r, depth)
        lat_s = lax.dot_general(qa_ref[r // inner, j, lax.rem(r, inner)], lat_buf[buf, j], NT_DIMS, preferred_element_type=jnp.float32)
        rope_s = jnp.dot(qr_ref[r // inner, j, lax.rem(r, inner)], rope_buf[buf, j], preferred_element_type=jnp.float32)
        return lat_s + rope_s

    def soften(r, j, raw):
        row = row_of(r, j)
        local = pos_ref[row] - me * slots
        slot = lax.broadcasted_iota(jnp.int32, (heads, slots), 1)
        qa, qr = qa_ref[r // inner, j, lax.rem(r, inner)], qr_ref[r // inner, j, lax.rem(r, inner)]
        s_new = (jnp.sum(qa.astype(jnp.float32) * cn_ref[pl.ds(row, 1), :], axis=-1, keepdims=True)
                 + jnp.sum(qr.astype(jnp.float32) * kn_ref[pl.ds(row, 1), :], axis=-1, keepdims=True)) * scale
        ok = slot < local
        hit = jnp.full((heads, 1), local, jnp.int32)
        hit = (hit >= 0) & (hit < slots)
        scores = jnp.where(ok, raw * scale, MASK_VALUE)
        s_new = jnp.where(hit, s_new, MASK_VALUE)
        top = jnp.maximum(jnp.max(scores, axis=-1, keepdims=True), s_new)
        weights = jnp.where(ok, jnp.exp(scores - top), 0.0)
        w_new = jnp.where(hit, jnp.exp(s_new - top), 0.0)
        den = jnp.sum(weights, axis=-1, keepdims=True) + w_new
        stats = pack_stats([top[g] for g in split], [den[g] for g in split], lane)
        return weights.astype(jnp.bfloat16), jnp.broadcast_to(w_new.astype(jnp.bfloat16).astype(jnp.float32), (heads, LANES)), stats

    def keep(r, soft):
        half = lax.rem(r, 2)
        for j, (weights, w_new, stats) in enumerate(soft):
            probs[half, j] = weights
            new_probs[half, j] = w_new
            part[r, j % 2, j // 2, tiles - 1] = stats

    def weigh(r, j):
        buf, half = lax.rem(r, depth), lax.rem(r, 2)
        lat_sum = jnp.dot(probs[half, j], lat_buf[buf, j], preferred_element_type=jnp.float32)
        w_new, c_new = new_probs[half, j], cn_ref[pl.ds(row_of(r, j), 1), :]
        for g in range(heads // SUBLANES):
            for n in range(rank // LANES):
                cols = slice(LANES * n, LANES * (n + 1))
                part[r, j % 2, j // 2, 4 * g + n] = lat_sum[split[g], cols] + w_new[split[g]] * c_new[:, cols]

    def put(dst, index, out, maxes, dens):
        for n in range(tiles - 1):
            dst[(*index, n)] = out[n]
        dst[(*index, tiles - 1)] = pack_stats(maxes, dens, lane)

    def merge_peer(r):
        for d in range(CHIPS):
            put(merged, (r, d), *merge_parts([[part[r, core, d, n] for n in range(tiles)], [peer_in[r, d, n] for n in range(tiles)]], lane))

    def merge_far(r):
        d = lax.rem(chip + direction(r) + CHIPS, CHIPS)
        put(relay, (r,), *merge_parts([[merged[r, d, n] for n in range(tiles)], [far_in[r, n] for n in range(tiles)]], lane))

    def merge_last(r):
        parts = [[merged[r, chip, n] for n in range(tiles)], [dir_in[r, n] for n in range(tiles)], [rel_in[r, n] for n in range(tiles)]]
        out, _, dens = merge_parts(parts, lane)
        rows = [jnp.concatenate([out[4 * g + n] / dens[g] for n in range(rank // LANES)], axis=-1) for g in range(heads // SUBLANES)]
        out_ref[r] = jnp.concatenate(rows, axis=0).astype(jnp.bfloat16)

    def start_sends(r):
        far_copy(r).start()
        dir_copy(r).start()

    def wait_last(r):
        dir_copy(r).wait()
        rel_copy(r).wait()

    for r in range(depth - 2):
        fetch(r)
    barrier = pltpu.get_barrier_semaphore()
    pl.semaphore_signal(barrier, inc=1, device_id={'sp': chip * 2 + 1 - core}, device_id_type=pl.DeviceIdType.MESH)
    pl.semaphore_signal(barrier, inc=1, device_id=at_chip(chip + 1), device_id_type=pl.DeviceIdType.MESH)
    pl.semaphore_signal(barrier, inc=1, device_id=at_chip(chip - 1), device_id_type=pl.DeviceIdType.MESH)
    pl.semaphore_wait(barrier, 3)

    def fetch_ahead(t):
        @pl.when(t < rounds - (depth - 2))
        def _():
            fetch(t + depth - 2)

    def edge_step(t, scoring):
        def stage(lag, *actions):
            @pl.when((t >= lag) & (t < rounds + lag))
            def _():
                for action in actions:
                    action(t - lag)

        if scoring:
            fetch_ahead(t)
            arrive(t)
            keep(t, [soften(t, j, score(t, j)) for j in range(owners)])
        stage(1, lambda r: [weigh(r, j) for j in range(owners)])
        stage(lag_peer, lambda r: peer_copy(r).wait(), merge_peer, start_sends)
        stage(lag_far, lambda r: far_copy(r).wait(), merge_far, lambda r: rel_copy(r).start())
        stage(lag_last, wait_last, merge_last)
        stage(1, lambda r: peer_copy(r).start())

    @pl.loop(0, lag_last)
    def _(t):
        edge_step(t, True)

    @pl.loop(lag_last, rounds)
    def _(t):
        fetch_ahead(t)
        arrive(t)
        peer_copy(t - lag_peer).wait()
        far_copy(t - lag_far).wait()
        wait_last(t - lag_last)
        merge_last(t - lag_last)
        merge_far(t - lag_far)
        merge_peer(t - lag_peer)
        raw = [score(t, j) for j in range(owners)]
        for j in range(owners):
            weigh(t - 1, j)
        keep(t, [soften(t, j, raw[j]) for j in range(owners)])
        start_sends(t - lag_peer)
        rel_copy(t - lag_far).start()
        peer_copy(t - 1).start()

    @pl.loop(rounds, rounds + lag_last)
    def _(t):
        edge_step(t, False)


def attend_shards(positions, lat, rope_t, q_abs, q_rope, lat_new, rope_new, scale, n_tp, n_sp):
    rows, slots, rank = lat.shape
    heads, rope_dim = q_rope.shape[1:]
    inner = rows // (n_tp * n_sp)
    rounds = rows // n_sp
    lags = (3, 7, 11)
    view = lambda a: a.reshape((n_tp, n_sp, inner) + a.shape[1:])

    tiles = (heads // SUBLANES) * (rank // LANES) + 1
    tile_set = (tiles, SUBLANES, LANES)
    vmem = lambda *lead: pltpu.VMEM(lead + tile_set, jnp.float32)
    sems = lambda n: pltpu.SemaphoreType.DMA((n,))
    rope_new = rope_new.astype(jnp.float32)
    return pl.pallas_call(
        functools.partial(attend_kernel, rounds, inner, lags, scale),
        in_specs=[pl.BlockSpec(memory_space=pltpu.SMEM)] + [pl.BlockSpec(memory_space=pltpu.VMEM)] * 4 + [pl.BlockSpec(memory_space=pl.ANY)] * 2,
        out_specs=pl.BlockSpec(memory_space=pltpu.VMEM),
        scratch_shapes=[
            pltpu.VMEM((LAT_DEPTH, n_sp, slots, rank), lat.dtype), pltpu.VMEM((LAT_DEPTH, n_sp, rope_dim, slots), rope_t.dtype),
            pltpu.VMEM((2, n_sp, heads, slots), jnp.bfloat16), pltpu.VMEM((2, n_sp, heads, LANES), jnp.float32),
            vmem(rounds, 2, CHIPS), vmem(rounds, CHIPS), vmem(rounds, CHIPS), vmem(rounds), vmem(rounds), vmem(rounds), vmem(rounds),
            sems(LAT_DEPTH), sems(LAT_DEPTH), sems(8), sems(8), sems(8), sems(8), sems(rounds), sems(rounds), sems(rounds), sems(rounds),
        ],
        out_shape=jax.ShapeDtypeStruct((rounds, heads, rank), jnp.bfloat16),
        compiler_params=pltpu.CompilerParams(collective_id=0, has_side_effects=True, vmem_limit_bytes=48 * 2 ** 20),
        name='attend',
    )(positions, view(q_abs), view(q_rope), lat_new, rope_new, view(lat), view(rope_t))


def project_kernel(chunks, cols, o_ref, w_ref, out_ref, w_buf, part, far_in, relay, dir_in, rel_in,
                   w_sem, far_send, dir_send, rel_send, far_recv, dir_recv, rel_recv):
    ring = CHIPS
    me = lax.axis_index('tp')
    depth = w_buf.shape[0]
    lag_far, lag_last = 2, 4

    def device(index):
        return {'tp': lax.rem(index + ring, ring)}

    def direction(n):
        return 1 - 2 * lax.rem(n, 2)

    def rows(index):
        return pl.ds(pl.multiple_of(lax.rem(index + ring, ring) * SUBLANES, SUBLANES), SUBLANES)

    def columns(n):
        return pl.ds(pl.multiple_of(n * cols, cols), cols)

    def remote(src, dst, send, recv, n, target):
        return pltpu.make_async_remote_copy(src_ref=src, dst_ref=dst.at[n], send_sem=send.at[n], recv_sem=recv.at[n],
                                            device_id=target, device_id_type=pl.DeviceIdType.MESH)

    def far_copy(n):
        return remote(part.at[n, rows(me + 2)], far_in, far_send, far_recv, n, device(me + direction(n)))

    def dir_copy(n):
        return remote(part.at[n, rows(me - direction(n))], dir_in, dir_send, dir_recv, n, device(me - direction(n)))

    def rel_copy(n):
        return remote(relay.at[n], rel_in, rel_send, rel_recv, n, device(me + direction(n)))

    def fetch(n):
        slot = lax.rem(n, depth)
        return pltpu.make_async_copy(w_ref.at[:, columns(n)], w_buf.at[slot], w_sem.at[slot])

    for n in range(depth - 1):
        fetch(n).start()
    barrier = pltpu.get_barrier_semaphore()
    pl.semaphore_signal(barrier, inc=1, device_id=device(me + 1), device_id_type=pl.DeviceIdType.MESH)
    pl.semaphore_signal(barrier, inc=1, device_id=device(me - 1), device_id_type=pl.DeviceIdType.MESH)
    pl.semaphore_wait(barrier, 2)

    @pl.loop(0, chunks + lag_last)
    def _(t):
        @pl.when(t < chunks - (depth - 1))
        def _():
            fetch(t + depth - 1).start()

        @pl.when(t < chunks)
        def _():
            fetch(t).wait()
            part[t] = jnp.dot(o_ref[...], w_buf[lax.rem(t, depth)], preferred_element_type=jnp.float32)

        @pl.when((t >= lag_last) & (t < chunks + lag_last))
        def _():
            n = t - lag_last
            dir_copy(n).wait()
            rel_copy(n).wait()
            out_ref[:, columns(n)] = part[n, rows(me)] + dir_in[n] + rel_in[n]

        @pl.when((t >= lag_far) & (t < chunks + lag_far))
        def _():
            n = t - lag_far
            far_copy(n).wait()
            relay[n] = part[n, rows(me + direction(n))] + far_in[n]

        @pl.when(t < chunks)
        def _():
            far_copy(t).start()
            dir_copy(t).start()

        @pl.when((t >= lag_far) & (t < chunks + lag_far))
        def _():
            rel_copy(t - lag_far).start()


def project_out(o_rows, w_out):
    rows, depth = o_rows.shape
    width = w_out.shape[1]
    cols = 1024
    chunks = width // cols
    block = lambda *lead: pltpu.VMEM(lead, jnp.float32)
    sems = pltpu.SemaphoreType.DMA((chunks,))
    return pl.pallas_call(
        functools.partial(project_kernel, chunks, cols),
        in_specs=[pl.BlockSpec(memory_space=pltpu.VMEM), pl.BlockSpec(memory_space=pl.ANY)],
        out_specs=pl.BlockSpec(memory_space=pltpu.VMEM),
        out_shape=jax.ShapeDtypeStruct((SUBLANES, width), jnp.float32),
        scratch_shapes=[
            pltpu.VMEM((4, depth, cols), w_out.dtype), block(chunks, rows, cols),
            block(chunks, SUBLANES, cols), block(chunks, SUBLANES, cols), block(chunks, SUBLANES, cols), block(chunks, SUBLANES, cols),
            pltpu.SemaphoreType.DMA((4,)), sems, sems, sems, sems, sems, sems,
        ],
        compiler_params=pltpu.CompilerParams(collective_id=1, has_side_effects=True, vmem_limit_bytes=28 * 2 ** 20),
        cost_estimate=pl.CostEstimate(flops=2 * rows * depth * width, bytes_accessed=2 * depth * width, transcendentals=0),
        name='project_out',
    )(o_rows, w_out)


def update_kernel(group, ahead, pos_ref, new_ref, col_ref, lat_ref, rope_ref, after_ref, lat_out, rope_out,
                  lat_buf, rope_buf, lat_in_sem, rope_in_sem, lat_out_sem, rope_out_sem):
    steps = lat_ref.shape[0] // group
    depth, _, slots, rank = lat_buf.shape
    slot_row = lax.broadcasted_iota(jnp.int32, (16, rank), 0)
    slot_col = lax.broadcasted_iota(jnp.int32, rope_buf.shape[2:], 1)

    def moves(i, inward):
        slot, rows = lax.rem(i, depth), pl.ds(i * group, group)
        if inward:
            return (pltpu.make_async_copy(lat_ref.at[rows], lat_buf.at[slot], lat_in_sem.at[slot]),
                    pltpu.make_async_copy(rope_ref.at[rows], rope_buf.at[slot], rope_in_sem.at[slot]))
        return (pltpu.make_async_copy(lat_buf.at[slot], lat_out.at[rows], lat_out_sem.at[slot]),
                pltpu.make_async_copy(rope_buf.at[slot], rope_out.at[rows], rope_out_sem.at[slot]))

    def start(i, inward):
        for move in moves(i, inward):
            move.start()

    def wait(i, inward):
        for move in moves(i, inward):
            move.wait()

    for i in range(ahead):
        start(i, True)

    @pl.loop(0, steps)
    def _(i):
        @pl.when((i + ahead < steps) & (i + ahead >= depth))
        def _():
            wait(i + ahead - depth, False)

        @pl.when(i + ahead < steps)
        def _():
            start(i + ahead, True)

        wait(i, True)
        slot = lax.rem(i, depth)
        for j in range(group):
            local = pos_ref[i * group + j]
            first = pl.multiple_of(jnp.clip(local, 0, slots - 1) // 16 * 16, 16)
            window = lat_buf[slot, j, pl.ds(first, 16), :].astype(jnp.float32)
            window = jnp.where(slot_row == local - first, new_ref[pl.ds(i * group + j, 1), :], window)
            lat_buf[slot, j, pl.ds(first, 16), :] = window.astype(lat_buf.dtype)
            rope = jnp.where(slot_col == local, col_ref[i, :, j:j + 1], rope_buf[slot, j].astype(jnp.float32))
            rope_buf[slot, j] = rope.astype(rope_buf.dtype)

        @pl.when(i >= 1)
        def _():
            start(i - 1, False)

    start(steps - 1, False)
    for i in range(steps - depth, steps):
        wait(i, False)


def update_caches(local_pos, lat, rope_t, lat_new, rope_new, after):
    rows, slots, rank = lat.shape
    rope_dim = rope_t.shape[1]
    group, depth, ahead = 8, 14, 7
    cols = rope_new.reshape(rows // group, group, rope_dim).swapaxes(1, 2)
    hbm = pl.BlockSpec(memory_space=pl.ANY)
    vmem = pl.BlockSpec(memory_space=pltpu.VMEM)
    sems = pltpu.SemaphoreType.DMA((depth,))
    return pl.pallas_call(
        functools.partial(update_kernel, group, ahead),
        in_specs=[pl.BlockSpec(memory_space=pltpu.SMEM), vmem, vmem, hbm, hbm, hbm],
        out_specs=[hbm, hbm],
        out_shape=[jax.ShapeDtypeStruct(lat.shape, lat.dtype), jax.ShapeDtypeStruct(rope_t.shape, rope_t.dtype)],
        scratch_shapes=[pltpu.VMEM((depth, group, slots, rank), lat.dtype), pltpu.VMEM((depth, group, rope_dim, slots), rope_t.dtype), sems, sems, sems, sems],
        compiler_params=pltpu.CompilerParams(vmem_limit_bytes=60 * 2 ** 20),
        cost_estimate=pl.CostEstimate(flops=50_000_000_000, bytes_accessed=4 * lat.size + 4 * rope_t.size, transcendentals=0),
        name='update_caches',
    )(local_pos, lat_new, cols, lat, rope_t, after)


def down_kernel(x_ref, wq_ref, wkv_ref, gq_ref, gkv_ref, cq_ref, lat_ref, rope_ref, acc_q, acc_kv):
    step = pl.program_id(0)
    rank = gkv_ref.shape[1]
    x = x_ref[...]
    part_q = jnp.dot(x, wq_ref[...], preferred_element_type=jnp.float32)
    part_kv = lax.dot_general(x, wkv_ref[...], NT_DIMS, preferred_element_type=jnp.float32)

    @pl.when(step == 0)
    def _():
        acc_q[...] = part_q
        acc_kv[...] = part_kv

    @pl.when(step > 0)
    def _():
        acc_q[...] += part_q
        acc_kv[...] += part_kv

    @pl.when(step == pl.num_programs(0) - 1)
    def _():
        h_q = acc_q[...].astype(jnp.bfloat16)
        cq_ref[...] = rms_norm(h_q, gq_ref[...]).astype(jnp.bfloat16)
        kv = acc_kv[...].astype(jnp.bfloat16)
        lat_ref[...] = rms_norm(kv[:, :rank], gkv_ref[...]).astype(jnp.bfloat16).astype(jnp.float32)
        rope_ref[...] = kv[:, rank:].astype(jnp.float32)


def project_down(hidden, w_dq, gain_q, w_dkv, gain_kv):
    rows, model = hidden.shape
    q_rank, kv_width, kv_rank = w_dq.shape[1], w_dkv.shape[1], gain_kv.shape[0]
    span = 1792
    whole = lambda *dims: pl.BlockSpec(dims, lambda k: (0,) * len(dims))
    return pl.pallas_call(
        down_kernel,
        grid=(model // span,),
        in_specs=[pl.BlockSpec((rows, span), lambda k: (0, k)), pl.BlockSpec((span, q_rank), lambda k: (k, 0)),
                  pl.BlockSpec((kv_width, span), lambda k: (0, k)), whole(1, q_rank), whole(1, kv_rank)],
        out_specs=[whole(rows, q_rank), whole(rows, kv_rank), whole(rows, kv_width - kv_rank)],
        out_shape=[jax.ShapeDtypeStruct((rows, q_rank), jnp.bfloat16), jax.ShapeDtypeStruct((rows, kv_rank), jnp.float32),
                   jax.ShapeDtypeStruct((rows, kv_width - kv_rank), jnp.float32)],
        scratch_shapes=[pltpu.VMEM((rows, q_rank), jnp.float32), pltpu.VMEM((rows, kv_width), jnp.float32)],
        compiler_params=pltpu.CompilerParams(vmem_limit_bytes=62 * 2 ** 20, dimension_semantics=('arbitrary',)),
        cost_estimate=pl.CostEstimate(flops=2 * rows * model * (q_rank + kv_width), bytes_accessed=2 * model * (q_rank + kv_width), transcendentals=0),
        name='project_down',
    )(hidden, w_dq, jnp.swapaxes(w_dkv, 0, 1), gain_q[None, :], gain_kv[None, :])


def solution(mesh):
    row_spec = P('dp', None)
    cache_spec = P('dp', 'sp', None)
    head_spec = P(None, 'tp', None)
    in_specs = (row_spec, cache_spec, cache_spec, P('dp'), P(), P(), P(), P(), head_spec, head_spec, head_spec, P('tp', None))
    out_specs = (row_spec, cache_spec, cache_spec)
    n_tp, n_sp = mesh.shape['tp'], mesh.shape['sp']

    def local_step(hidden, lat_cache, rope_cache, positions, w_dq, gain_q, w_dkv, gain_kv, w_uq, w_uk, w_uv, w_out):
        seq_local = lat_cache.shape[1]
        score_scale = YARN_MSCALE ** 2 / math.sqrt(w_uq.shape[2])
        q_abs, q_rope, lat_new, rope_new = project_inputs(hidden, positions, w_dq, gain_q, w_dkv, gain_kv, w_uq, w_uk)
        rope_t = jnp.swapaxes(rope_cache, 1, 2)
        o_lat = attend_shards(positions, lat_cache, rope_t, q_abs, q_rope, lat_new, rope_new, score_scale, n_tp, n_sp)
        o_heads = jnp.einsum('bhk,khv->bhv', o_lat, w_uv, preferred_element_type=jnp.float32).astype(jnp.bfloat16)
        attn_rows = project_out(o_heads.reshape(o_heads.shape[0], -1), w_out)
        attn_out = lax.all_gather(attn_rows, ('tp', 'sp'), axis=0, tiled=True)
        local_pos = positions - lax.axis_index('sp') * seq_local
        lat_all, rope_all = update_caches(local_pos, lat_cache, rope_t, lat_new, rope_new.astype(jnp.float32), attn_rows)
        return (hidden.astype(jnp.float32) + attn_out).astype(jnp.bfloat16), lat_all, jnp.swapaxes(rope_all, 1, 2)

    return jax.shard_map(local_step, mesh=mesh, in_specs=in_specs, out_specs=out_specs, check_vma=False)
```

```python
import functools
import math
import jax
import jax.numpy as jnp
from jax import lax
from jax.experimental import pallas as pl
from jax.experimental.pallas import tpu as pltpu
from jax.sharding import PartitionSpec as P

EPSILON = 1e-6
ROPE_BASE = 50000.0
YARN_MSCALE = 1.0 + 0.1 * math.log(32.0)
MASK_VALUE = -1e30
LAT_DEPTH = 5
CHIPS = 4
SUBLANES = 8
LANES = 128
NT_DIMS = (((1,), (1,)), ((), ()))


def rms_norm(values, gain):
    vals32 = values.astype(jnp.float32)
    inv_rms = lax.rsqrt(jnp.mean(vals32 * vals32, axis=-1, keepdims=True) + EPSILON)
    return vals32 * inv_rms * gain.astype(jnp.float32)


def rope_tables(positions, rope_dim):
    half_dim = rope_dim // 2
    inv_freq = ROPE_BASE ** (-jnp.arange(half_dim).astype(jnp.float32) / half_dim)
    angles = positions.astype(jnp.float32)[:, None] * inv_freq[None, :]
    return jnp.cos(angles), jnp.sin(angles)


def rotate_pairs(values, cos_t, sin_t):
    half_dim = values.shape[-1] // 2
    first_half = values[..., :half_dim]
    second_half = values[..., half_dim:]
    return jnp.concatenate([first_half * cos_t - second_half * sin_t, second_half * cos_t + first_half * sin_t], axis=-1)


def project_inputs(hidden, positions, w_dq, gain_q, w_dkv, gain_kv, w_uq, w_uk):
    nope_dim = w_uk.shape[2]
    cos_t, sin_t = rope_tables(positions, w_uq.shape[2] - nope_dim)
    c_q, lat_new, k_rope = project_down(hidden, w_dq, gain_q, w_dkv, gain_kv)
    q_full = jnp.einsum('br,rhd->bhd', c_q, w_uq, preferred_element_type=jnp.float32).astype(jnp.bfloat16)
    q_rope = rotate_pairs(q_full[:, :, nope_dim:].astype(jnp.float32), cos_t[:, None, :], sin_t[:, None, :]).astype(jnp.bfloat16)
    q_rope = jnp.transpose(lax.optimization_barrier(jnp.transpose(q_rope, (1, 2, 0))), (2, 0, 1))
    q_abs = jnp.einsum('bhn,khn->bhk', q_full[:, :, :nope_dim], w_uk, preferred_element_type=jnp.float32).astype(jnp.bfloat16)
    rope_new = rotate_pairs(k_rope, cos_t, sin_t).astype(jnp.bfloat16)
    return q_abs, q_rope, lat_new, rope_new


def merge_parts(parts, lane):
    groups = len(parts[0]) // 4
    stats = [p[-1] for p in parts]
    out, maxes, dens = [], [], []
    for g in range(groups):
        ms = [jnp.broadcast_to(s[:, 2 * g:2 * g + 1], s.shape) for s in stats]
        ls = [jnp.broadcast_to(s[:, 2 * g + 1:2 * g + 2], s.shape) for s in stats]
        top = functools.reduce(jnp.maximum, ms)
        ws = [jnp.exp(m - top) for m in ms]
        maxes.append(top)
        dens.append(sum(w * l for w, l in zip(ws, ls)))
        for n in range(4):
            out.append(sum(w * p[4 * g + n] for w, p in zip(ws, parts)))
    return out, maxes, dens


def pack_stats(maxes, dens, lane):
    tile = jnp.zeros((SUBLANES, LANES), jnp.float32)
    for g, (m, l) in enumerate(zip(maxes, dens)):
        tile = jnp.where(lane == 2 * g, m, tile)
        tile = jnp.where(lane == 2 * g + 1, l, tile)
    return tile


def attend_kernel(rounds, inner, lags, scale, pos_ref, qa_ref, qr_ref, cn_ref, kn_ref, lat_ref, rope_ref, out_ref,
                  lat_buf, rope_buf, probs, new_probs, part, peer_in, merged, far_in, relay, dir_in, rel_in,
                  lat_sem, rope_sem, peer_send, far_send, dir_send, rel_send, peer_recv, far_recv, dir_recv, rel_recv):
    me = lax.axis_index('sp')
    chip, core = me // 2, lax.rem(me, 2)
    owners = lat_ref.shape[1]
    slots = lat_ref.shape[3]
    heads, rank = qa_ref.shape[3], qa_ref.shape[4]
    lane = lax.broadcasted_iota(jnp.int32, (SUBLANES, LANES), 1)
    tiles = part.shape[3]
    depth = lat_buf.shape[0]
    split = [slice(SUBLANES * g, SUBLANES * (g + 1)) for g in range(heads // SUBLANES)]
    lag_peer, lag_far, lag_last = lags

    def at_chip(index):
        return {'sp': lax.rem(index + CHIPS, CHIPS) * 2 + core}

    def direction(r):
        return 1 - 2 * lax.rem(r, 2)

    def remote(src, dst, send, recv, r, target):
        return pltpu.make_async_remote_copy(
            src_ref=src, dst_ref=dst.at[r], send_sem=send.at[lax.rem(r, send.shape[0])], recv_sem=recv.at[r],
            device_id=target, device_id_type=pl.DeviceIdType.MESH)

    def peer_copy(r):
        return remote(part.at[r, 1 - core], peer_in, peer_send, peer_recv, r, {'sp': chip * 2 + 1 - core})

    def far_copy(r):
        return remote(merged.at[r, lax.rem(chip + 2, CHIPS)], far_in, far_send, far_recv, r, at_chip(chip + direction(r)))

    def dir_copy(r):
        source = lax.rem(chip - direction(r) + CHIPS, CHIPS)
        return remote(merged.at[r, source], dir_in, dir_send, dir_recv, r, at_chip(chip - direction(r)))

    def rel_copy(r):
        return remote(relay.at[r], rel_in, rel_send, rel_recv, r, at_chip(chip + direction(r)))

    def lat_copy(r):
        slot = lax.rem(r, depth)
        return pltpu.make_async_copy(lat_ref.at[r // inner, :, lax.rem(r, inner)], lat_buf.at[slot], lat_sem.at[slot])

    def rope_copy(r):
        slot = lax.rem(r, depth)
        return pltpu.make_async_copy(rope_ref.at[r // inner, :, lax.rem(r, inner)], rope_buf.at[slot], rope_sem.at[slot])

    def fetch(r):
        lat_copy(r).start()
        rope_copy(r).start()

    def arrive(r):
        lat_copy(r).wait()
        rope_copy(r).wait()

    def row_of(r, j):
        return (r // inner) * (owners * inner) + j * inner + lax.rem(r, inner)

    def score(r, j):
        buf = lax.rem(r, depth)
        lat_s = lax.dot_general(qa_ref[r // inner, j, lax.rem(r, inner)], lat_buf[buf, j], NT_DIMS, preferred_element_type=jnp.float32)
        rope_s = jnp.dot(qr_ref[r // inner, j, lax.rem(r, inner)], rope_buf[buf, j], preferred_element_type=jnp.float32)
        return lat_s + rope_s

    def soften(r, j, raw):
        row = row_of(r, j)
        local = pos_ref[row] - me * slots
        slot = lax.broadcasted_iota(jnp.int32, (heads, slots), 1)
        qa, qr = qa_ref[r // inner, j, lax.rem(r, inner)], qr_ref[r // inner, j, lax.rem(r, inner)]
        s_new = (jnp.sum(qa.astype(jnp.float32) * cn_ref[pl.ds(row, 1), :], axis=-1, keepdims=True)
                 + jnp.sum(qr.astype(jnp.float32) * kn_ref[pl.ds(row, 1), :], axis=-1, keepdims=True)) * scale
        ok = slot < local
        hit = jnp.full((heads, 1), local, jnp.int32)
        hit = (hit >= 0) & (hit < slots)
        scores = jnp.where(ok, raw * scale, MASK_VALUE)
        s_new = jnp.where(hit, s_new, MASK_VALUE)
        top = jnp.maximum(jnp.max(scores, axis=-1, keepdims=True), s_new)
        weights = jnp.where(ok, jnp.exp(scores - top), 0.0)
        w_new = jnp.where(hit, jnp.exp(s_new - top), 0.0)
        den = jnp.sum(weights, axis=-1, keepdims=True) + w_new
        stats = pack_stats([top[g] for g in split], [den[g] for g in split], lane)
        return weights.astype(jnp.bfloat16), jnp.broadcast_to(w_new.astype(jnp.bfloat16).astype(jnp.float32), (heads, LANES)), stats

    def keep(r, soft):
        half = lax.rem(r, 2)
        for j, (weights, w_new, stats) in enumerate(soft):
            probs[half, j] = weights
            new_probs[half, j] = w_new
            part[r, j % 2, j // 2, tiles - 1] = stats

    def weigh(r, j):
        buf, half = lax.rem(r, depth), lax.rem(r, 2)
        lat_sum = jnp.dot(probs[half, j], lat_buf[buf, j], preferred_element_type=jnp.float32)
        w_new, c_new = new_probs[half, j], cn_ref[pl.ds(row_of(r, j), 1), :]
        for g in range(heads // SUBLANES):
            for n in range(rank // LANES):
                cols = slice(LANES * n, LANES * (n + 1))
                part[r, j % 2, j // 2, 4 * g + n] = lat_sum[split[g], cols] + w_new[split[g]] * c_new[:, cols]

    def put(dst, index, out, maxes, dens):
        for n in range(tiles - 1):
            dst[(*index, n)] = out[n]
        dst[(*index, tiles - 1)] = pack_stats(maxes, dens, lane)

    def merge_peer(r):
        for d in range(CHIPS):
            put(merged, (r, d), *merge_parts([[part[r, core, d, n] for n in range(tiles)], [peer_in[r, d, n] for n in range(tiles)]], lane))

    def merge_far(r):
        d = lax.rem(chip + direction(r) + CHIPS, CHIPS)
        put(relay, (r,), *merge_parts([[merged[r, d, n] for n in range(tiles)], [far_in[r, n] for n in range(tiles)]], lane))

    def merge_last(r):
        parts = [[merged[r, chip, n] for n in range(tiles)], [dir_in[r, n] for n in range(tiles)], [rel_in[r, n] for n in range(tiles)]]
        out, _, dens = merge_parts(parts, lane)
        rows = [jnp.concatenate([out[4 * g + n] / dens[g] for n in range(rank // LANES)], axis=-1) for g in range(heads // SUBLANES)]
        out_ref[r] = jnp.concatenate(rows, axis=0).astype(jnp.bfloat16)

    def start_sends(r):
        far_copy(r).start()
        dir_copy(r).start()

    def wait_last(r):
        dir_copy(r).wait()
        rel_copy(r).wait()

    for r in range(depth - 2):
        fetch(r)
    barrier = pltpu.get_barrier_semaphore()
    pl.semaphore_signal(barrier, inc=1, device_id={'sp': chip * 2 + 1 - core}, device_id_type=pl.DeviceIdType.MESH)
    pl.semaphore_signal(barrier, inc=1, device_id=at_chip(chip + 1), device_id_type=pl.DeviceIdType.MESH)
    pl.semaphore_signal(barrier, inc=1, device_id=at_chip(chip - 1), device_id_type=pl.DeviceIdType.MESH)
    pl.semaphore_wait(barrier, 3)

    def fetch_ahead(t):
        @pl.when(t < rounds - (depth - 2))
        def _():
            fetch(t + depth - 2)

    def edge_step(t, scoring):
        def stage(lag, *actions):
            @pl.when((t >= lag) & (t < rounds + lag))
            def _():
                for action in actions:
                    action(t - lag)

        if scoring:
            fetch_ahead(t)
            arrive(t)
            keep(t, [soften(t, j, score(t, j)) for j in range(owners)])
        stage(1, lambda r: [weigh(r, j) for j in range(owners)])
        stage(lag_peer, lambda r: peer_copy(r).wait(), merge_peer, start_sends)
        stage(lag_far, lambda r: far_copy(r).wait(), merge_far, lambda r: rel_copy(r).start())
        stage(lag_last, wait_last, merge_last)
        stage(1, lambda r: peer_copy(r).start())

    @pl.loop(0, lag_last)
    def _(t):
        edge_step(t, True)

    @pl.loop(lag_last, rounds)
    def _(t):
        fetch_ahead(t)
        arrive(t)
        peer_copy(t - lag_peer).wait()
        far_copy(t - lag_far).wait()
        wait_last(t - lag_last)
        merge_last(t - lag_last)
        merge_far(t - lag_far)
        merge_peer(t - lag_peer)
        raw = [score(t, j) for j in range(owners)]
        for j in range(owners):
            weigh(t - 1, j)
        keep(t, [soften(t, j, raw[j]) for j in range(owners)])
        start_sends(t - lag_peer)
        rel_copy(t - lag_far).start()
        peer_copy(t - 1).start()

    @pl.loop(rounds, rounds + lag_last)
    def _(t):
        edge_step(t, False)


def attend_shards(positions, lat, rope_t, q_abs, q_rope, lat_new, rope_new, scale, n_tp, n_sp):
    rows, slots, rank = lat.shape
    heads, rope_dim = q_rope.shape[1:]
    inner = rows // (n_tp * n_sp)
    rounds = rows // n_sp
    lags = (4, 9, 14)
    view = lambda a: a.reshape((n_tp, n_sp, inner) + a.shape[1:])

    tiles = (heads // SUBLANES) * (rank // LANES) + 1
    tile_set = (tiles, SUBLANES, LANES)
    vmem = lambda *lead: pltpu.VMEM(lead + tile_set, jnp.float32)
    sems = lambda n: pltpu.SemaphoreType.DMA((n,))
    rope_new = rope_new.astype(jnp.float32)
    return pl.pallas_call(
        functools.partial(attend_kernel, rounds, inner, lags, scale),
        in_specs=[pl.BlockSpec(memory_space=pltpu.SMEM)] + [pl.BlockSpec(memory_space=pltpu.VMEM)] * 4 + [pl.BlockSpec(memory_space=pl.ANY)] * 2,
        out_specs=pl.BlockSpec(memory_space=pltpu.VMEM),
        scratch_shapes=[
            pltpu.VMEM((LAT_DEPTH, n_sp, slots, rank), lat.dtype), pltpu.VMEM((LAT_DEPTH, n_sp, rope_dim, slots), rope_t.dtype),
            pltpu.VMEM((2, n_sp, heads, slots), jnp.bfloat16), pltpu.VMEM((2, n_sp, heads, LANES), jnp.float32),
            vmem(rounds, 2, CHIPS), vmem(rounds, CHIPS), vmem(rounds, CHIPS), vmem(rounds), vmem(rounds), vmem(rounds), vmem(rounds),
            sems(LAT_DEPTH), sems(LAT_DEPTH), sems(8), sems(8), sems(8), sems(8), sems(rounds), sems(rounds), sems(rounds), sems(rounds),
        ],
        out_shape=jax.ShapeDtypeStruct((rounds, heads, rank), jnp.bfloat16),
        compiler_params=pltpu.CompilerParams(collective_id=0, has_side_effects=True, vmem_limit_bytes=48 * 2 ** 20),
        name='attend',
    )(positions, view(q_abs), view(q_rope), lat_new, rope_new, view(lat), view(rope_t))


def project_kernel(chunks, cols, o_ref, w_ref, out_ref, w_buf, part, far_in, relay, dir_in, rel_in,
                   w_sem, far_send, dir_send, rel_send, far_recv, dir_recv, rel_recv):
    ring = CHIPS
    me = lax.axis_index('tp')
    depth = w_buf.shape[0]
    lag_far, lag_last = 2, 4

    def device(index):
        return {'tp': lax.rem(index + ring, ring)}

    def direction(n):
        return 1 - 2 * lax.rem(n, 2)

    def rows(index):
        return pl.ds(pl.multiple_of(lax.rem(index + ring, ring) * SUBLANES, SUBLANES), SUBLANES)

    def columns(n):
        return pl.ds(pl.multiple_of(n * cols, cols), cols)

    def remote(src, dst, send, recv, n, target):
        return pltpu.make_async_remote_copy(src_ref=src, dst_ref=dst.at[n], send_sem=send.at[n], recv_sem=recv.at[n],
                                            device_id=target, device_id_type=pl.DeviceIdType.MESH)

    def far_copy(n):
        return remote(part.at[n, rows(me + 2)], far_in, far_send, far_recv, n, device(me + direction(n)))

    def dir_copy(n):
        return remote(part.at[n, rows(me - direction(n))], dir_in, dir_send, dir_recv, n, device(me - direction(n)))

    def rel_copy(n):
        return remote(relay.at[n], rel_in, rel_send, rel_recv, n, device(me + direction(n)))

    def fetch(n):
        slot = lax.rem(n, depth)
        return pltpu.make_async_copy(w_ref.at[:, columns(n)], w_buf.at[slot], w_sem.at[slot])

    for n in range(depth - 1):
        fetch(n).start()
    barrier = pltpu.get_barrier_semaphore()
    pl.semaphore_signal(barrier, inc=1, device_id=device(me + 1), device_id_type=pl.DeviceIdType.MESH)
    pl.semaphore_signal(barrier, inc=1, device_id=device(me - 1), device_id_type=pl.DeviceIdType.MESH)
    pl.semaphore_wait(barrier, 2)

    @pl.loop(0, chunks + lag_last)
    def _(t):
        @pl.when(t < chunks - (depth - 1))
        def _():
            fetch(t + depth - 1).start()

        @pl.when(t < chunks)
        def _():
            fetch(t).wait()
            part[t] = jnp.dot(o_ref[...], w_buf[lax.rem(t, depth)], preferred_element_type=jnp.float32)

        @pl.when((t >= lag_last) & (t < chunks + lag_last))
        def _():
            n = t - lag_last
            dir_copy(n).wait()
            rel_copy(n).wait()
            out_ref[:, columns(n)] = part[n, rows(me)] + dir_in[n] + rel_in[n]

        @pl.when((t >= lag_far) & (t < chunks + lag_far))
        def _():
            n = t - lag_far
            far_copy(n).wait()
            relay[n] = part[n, rows(me + direction(n))] + far_in[n]

        @pl.when(t < chunks)
        def _():
            far_copy(t).start()
            dir_copy(t).start()

        @pl.when((t >= lag_far) & (t < chunks + lag_far))
        def _():
            rel_copy(t - lag_far).start()


def project_out(o_rows, w_out):
    rows, depth = o_rows.shape
    width = w_out.shape[1]
    cols = 1024
    chunks = width // cols
    block = lambda *lead: pltpu.VMEM(lead, jnp.float32)
    sems = pltpu.SemaphoreType.DMA((chunks,))
    return pl.pallas_call(
        functools.partial(project_kernel, chunks, cols),
        in_specs=[pl.BlockSpec(memory_space=pltpu.VMEM), pl.BlockSpec(memory_space=pl.ANY)],
        out_specs=pl.BlockSpec(memory_space=pltpu.VMEM),
        out_shape=jax.ShapeDtypeStruct((SUBLANES, width), jnp.float32),
        scratch_shapes=[
            pltpu.VMEM((4, depth, cols), w_out.dtype), block(chunks, rows, cols),
            block(chunks, SUBLANES, cols), block(chunks, SUBLANES, cols), block(chunks, SUBLANES, cols), block(chunks, SUBLANES, cols),
            pltpu.SemaphoreType.DMA((4,)), sems, sems, sems, sems, sems, sems,
        ],
        compiler_params=pltpu.CompilerParams(collective_id=1, has_side_effects=True, vmem_limit_bytes=28 * 2 ** 20),
        cost_estimate=pl.CostEstimate(flops=2 * rows * depth * width, bytes_accessed=2 * depth * width, transcendentals=0),
        name='project_out',
    )(o_rows, w_out)


def update_kernel(group, ahead, pos_ref, new_ref, col_ref, lat_ref, rope_ref, after_ref, lat_out, rope_out,
                  lat_buf, rope_buf, lat_in_sem, rope_in_sem, lat_out_sem, rope_out_sem):
    steps = lat_ref.shape[0] // group
    depth, _, slots, rank = lat_buf.shape
    slot_row = lax.broadcasted_iota(jnp.int32, (16, rank), 0)
    slot_col = lax.broadcasted_iota(jnp.int32, rope_buf.shape[2:], 1)

    def moves(i, inward):
        slot, rows = lax.rem(i, depth), pl.ds(i * group, group)
        if inward:
            return (pltpu.make_async_copy(lat_ref.at[rows], lat_buf.at[slot], lat_in_sem.at[slot]),
                    pltpu.make_async_copy(rope_ref.at[rows], rope_buf.at[slot], rope_in_sem.at[slot]))
        return (pltpu.make_async_copy(lat_buf.at[slot], lat_out.at[rows], lat_out_sem.at[slot]),
                pltpu.make_async_copy(rope_buf.at[slot], rope_out.at[rows], rope_out_sem.at[slot]))

    def start(i, inward):
        for move in moves(i, inward):
            move.start()

    def wait(i, inward):
        for move in moves(i, inward):
            move.wait()

    for i in range(ahead):
        start(i, True)

    @pl.loop(0, steps)
    def _(i):
        @pl.when((i + ahead < steps) & (i + ahead >= depth))
        def _():
            wait(i + ahead - depth, False)

        @pl.when(i + ahead < steps)
        def _():
            start(i + ahead, True)

        wait(i, True)
        slot = lax.rem(i, depth)
        for j in range(group):
            local = pos_ref[i * group + j]
            first = pl.multiple_of(jnp.clip(local, 0, slots - 1) // 16 * 16, 16)
            window = lat_buf[slot, j, pl.ds(first, 16), :].astype(jnp.float32)
            window = jnp.where(slot_row == local - first, new_ref[pl.ds(i * group + j, 1), :], window)
            lat_buf[slot, j, pl.ds(first, 16), :] = window.astype(lat_buf.dtype)
            rope = jnp.where(slot_col == local, col_ref[i, :, j:j + 1], rope_buf[slot, j].astype(jnp.float32))
            rope_buf[slot, j] = rope.astype(rope_buf.dtype)

        @pl.when(i >= 1)
        def _():
            start(i - 1, False)

    start(steps - 1, False)
    for i in range(steps - depth, steps):
        wait(i, False)


def update_caches(local_pos, lat, rope_t, lat_new, rope_new, after):
    rows, slots, rank = lat.shape
    rope_dim = rope_t.shape[1]
    group, depth, ahead = 8, 14, 7
    cols = rope_new.reshape(rows // group, group, rope_dim).swapaxes(1, 2)
    hbm = pl.BlockSpec(memory_space=pl.ANY)
    vmem = pl.BlockSpec(memory_space=pltpu.VMEM)
    sems = pltpu.SemaphoreType.DMA((depth,))
    return pl.pallas_call(
        functools.partial(update_kernel, group, ahead),
        in_specs=[pl.BlockSpec(memory_space=pltpu.SMEM), vmem, vmem, hbm, hbm, hbm],
        out_specs=[hbm, hbm],
        out_shape=[jax.ShapeDtypeStruct(lat.shape, lat.dtype), jax.ShapeDtypeStruct(rope_t.shape, rope_t.dtype)],
        scratch_shapes=[pltpu.VMEM((depth, group, slots, rank), lat.dtype), pltpu.VMEM((depth, group, rope_dim, slots), rope_t.dtype), sems, sems, sems, sems],
        compiler_params=pltpu.CompilerParams(vmem_limit_bytes=60 * 2 ** 20),
        cost_estimate=pl.CostEstimate(flops=50_000_000_000, bytes_accessed=4 * lat.size + 4 * rope_t.size, transcendentals=0),
        name='update_caches',
    )(local_pos, lat_new, cols, lat, rope_t, after)


def down_kernel(x_ref, wq_ref, wkv_ref, gain_ref, cq_ref, lat_ref, rope_ref, acc_q, acc_kv):
    step = pl.program_id(0)
    q_rank, rank = cq_ref.shape[1], lat_ref.shape[1]
    x = x_ref[...]
    part_q = jnp.dot(x, wq_ref[...], preferred_element_type=jnp.float32)
    part_kv = lax.dot_general(x, wkv_ref[...], NT_DIMS, preferred_element_type=jnp.float32)

    @pl.when(step == 0)
    def _():
        acc_q[...] = part_q
        acc_kv[...] = part_kv

    @pl.when(step > 0)
    def _():
        acc_q[...] += part_q
        acc_kv[...] += part_kv

    @pl.when(step == pl.num_programs(0) - 1)
    def _():
        h_q = acc_q[...].astype(jnp.bfloat16)
        cq_ref[...] = rms_norm(h_q, gain_ref[:, :q_rank]).astype(jnp.bfloat16)
        kv = acc_kv[...].astype(jnp.bfloat16)
        lat_ref[...] = rms_norm(kv[:, :rank], gain_ref[:, q_rank:]).astype(jnp.bfloat16).astype(jnp.float32)
        rope_ref[...] = kv[:, rank:].astype(jnp.float32)


def project_down(hidden, w_dq, gain_q, w_dkv, gain_kv):
    rows, model = hidden.shape
    q_rank, kv_width, kv_rank = w_dq.shape[1], w_dkv.shape[1], gain_kv.shape[0]
    span = 1792
    whole = lambda *dims: pl.BlockSpec(dims, lambda k: (0,) * len(dims))
    return pl.pallas_call(
        down_kernel,
        grid=(model // span,),
        in_specs=[pl.BlockSpec((rows, span), lambda k: (0, k)), pl.BlockSpec((span, q_rank), lambda k: (k, 0)),
                  pl.BlockSpec((kv_width, span), lambda k: (0, k)), whole(1, q_rank + kv_rank)],
        out_specs=[whole(rows, q_rank), whole(rows, kv_rank), whole(rows, kv_width - kv_rank)],
        out_shape=[jax.ShapeDtypeStruct((rows, q_rank), jnp.bfloat16), jax.ShapeDtypeStruct((rows, kv_rank), jnp.float32),
                   jax.ShapeDtypeStruct((rows, kv_width - kv_rank), jnp.float32)],
        scratch_shapes=[pltpu.VMEM((rows, q_rank), jnp.float32), pltpu.VMEM((rows, kv_width), jnp.float32)],
        compiler_params=pltpu.CompilerParams(vmem_limit_bytes=62 * 2 ** 20, dimension_semantics=('arbitrary',)),
        cost_estimate=pl.CostEstimate(flops=2 * rows * model * (q_rank + kv_width), bytes_accessed=2 * model * (q_rank + kv_width), transcendentals=0),
        name='project_down',
    )(hidden, w_dq, jnp.swapaxes(w_dkv, 0, 1), jnp.concatenate([gain_q, gain_kv])[None, :])


def solution(mesh):
    row_spec = P('dp', None)
    cache_spec = P('dp', 'sp', None)
    head_spec = P(None, 'tp', None)
    in_specs = (row_spec, cache_spec, cache_spec, P('dp'), P(), P(), P(), P(), head_spec, head_spec, head_spec, P('tp', None))
    out_specs = (row_spec, cache_spec, cache_spec)
    n_tp, n_sp = mesh.shape['tp'], mesh.shape['sp']

    def local_step(hidden, lat_cache, rope_cache, positions, w_dq, gain_q, w_dkv, gain_kv, w_uq, w_uk, w_uv, w_out):
        seq_local = lat_cache.shape[1]
        score_scale = YARN_MSCALE ** 2 / math.sqrt(w_uq.shape[2])
        q_abs, q_rope, lat_new, rope_new = project_inputs(hidden, positions, w_dq, gain_q, w_dkv, gain_kv, w_uq, w_uk)
        rope_t = jnp.swapaxes(rope_cache, 1, 2)
        o_lat = attend_shards(positions, lat_cache, rope_t, q_abs, q_rope, lat_new, rope_new, score_scale, n_tp, n_sp)
        o_heads = jnp.einsum('bhk,khv->bhv', o_lat, w_uv, preferred_element_type=jnp.float32).astype(jnp.bfloat16)
        attn_rows = project_out(o_heads.reshape(o_heads.shape[0], -1), w_out)
        attn_out = lax.all_gather(attn_rows, ('tp', 'sp'), axis=0, tiled=True)
        local_pos = positions - lax.axis_index('sp') * seq_local
        lat_all, rope_all = update_caches(local_pos, lat_cache, rope_t, lat_new, rope_new.astype(jnp.float32), attn_rows)
        return (hidden.astype(jnp.float32) + attn_out).astype(jnp.bfloat16), lat_all, jnp.swapaxes(rope_all, 1, 2)

    return jax.shard_map(local_step, mesh=mesh, in_specs=in_specs, out_specs=out_specs, check_vma=False)
```
